32 devices in a mesh: dp: 2 (over x), tp: 16 (over y, z, core).
Axes of the slice: x: 2, y: 2, z: 4, core: 2. Of those that a mesh axis runs over, the one named last changes fastest.
Arguments:
- x: bfloat16 [11264, 3072], P(('dp', 'tp')), parts along dimension 0
- dy: bfloat16 [11264, 3072], P(('dp', 'tp')), parts along dimension 0
- gate: bfloat16 [11264, 24576], P('dp', 'tp'), parts along dimension 0
- up: bfloat16 [11264, 24576], P('dp', 'tp'), parts along dimension 0
- w_gate: bfloat16 [3072, 24576], P(None, 'tp')
- w_up: bfloat16 [3072, 24576], P(None, 'tp')
- w_down: bfloat16 [24576, 3072], P('tp')
Outputs:
- output 1: bfloat16 [11264, 3072], P(('dp', 'tp')), parts along dimension 0
- output 2: bfloat16 [6144, 24576], P('dp', 'tp'), parts along dimension 0
- output 3: bfloat16 [6144, 24576], P('dp', 'tp'), parts along dimension 0
- output 4: bfloat16 [49152, 3072], P(('dp', 'tp')), parts along dimension 0
There are 2 independent parts. The reference program is written for one: setup_inputs(seed, part) draws one part's arguments, and reference() takes and returns one part's arrays. A program takes and returns all parts, laid end to end along the dimension named above; an argument that names none is the same for every part.
All inputs are finite; a program needn't handle non-finite values.
Results may differ from the reference program's by a relative error of at most 0.012.
Values are sent between devices in bfloat16 or wider.
A program may use at most 2 GiB of HBM per device.

```python
import jax
import jax.numpy as jnp

ROWS = 5632
D = 3072
FF = 24576


def act(gate, up):
    return jax.nn.gelu(gate) * up


def setup_inputs(seed: int = 0, part: int = 0) -> dict:
    kx, ky, ka, kb, kg, ku, kd = jax.random.split(jax.random.key(seed), 7)
    kx, ky, ka, kb = (jax.random.fold_in(k, part) for k in (kx, ky, ka, kb))
    drawn = {
        "x": jax.random.normal(kx, (ROWS, D), jnp.float32),
        "dy": jax.random.normal(ky, (ROWS, D), jnp.float32),
        "gate": jax.random.normal(ka, (ROWS, FF), jnp.float32),
        "up": jax.random.normal(kb, (ROWS, FF), jnp.float32),
        "w_gate": jax.random.normal(kg, (D, FF), jnp.float32) * D**-0.5,
        "w_up": jax.random.normal(ku, (D, FF), jnp.float32) * D**-0.5,
        "w_down": jax.random.normal(kd, (FF, D), jnp.float32) * FF**-0.5,
    }
    return {k: v.astype(jnp.bfloat16) for k, v in drawn.items()}


def reference(x, dy, gate, up, w_gate, w_up, w_down):
    hidden, back = jax.vjp(act, gate.astype(jnp.float32), up.astype(jnp.float32))
    d_hidden = jnp.dot(dy, w_down.T, preferred_element_type=jnp.float32)
    d_gate, d_up = (g.astype(jnp.bfloat16) for g in back(d_hidden))
    dx = jnp.dot(d_gate, w_gate.T, preferred_element_type=jnp.float32) + jnp.dot(d_up, w_up.T, preferred_element_type=jnp.float32)
    dw_gate = jnp.dot(x.T, d_gate, preferred_element_type=jnp.float32)
    dw_up = jnp.dot(x.T, d_up, preferred_element_type=jnp.float32)
    dw_down = jnp.dot(hidden.astype(jnp.bfloat16).T, dy, preferred_element_type=jnp.float32)
    return tuple(g.astype(jnp.bfloat16) for g in (dx, dw_gate, dw_up, dw_down))
```

```python
import jax
import jax.numpy as jnp
from jax import lax
from jax.experimental import pallas as pl
from jax.experimental.pallas import tpu as pltpu
from jax.sharding import PartitionSpec as P

R, D, F = 352, 3072, 1536
H = R // 2
RING = 8
NC = 2
CH = F
BF, F32 = jnp.bfloat16, jnp.float32
NT = (((1,), (1,)), ((), ()))
PARTS = ((0, 96), (96, 80), (176, 96), (272, 80))
C0, C1 = 0.7978845608028654, 0.044715
TILE = 512


def grads(g, u, dh):
    g, u = g.astype(F32), u.astype(F32)
    g2 = g * g
    t = jnp.tanh(C0 * (g * (1.0 + C1 * g2)))
    q = 0.5 * (1.0 + t)
    gelu = g * q
    slope = q + (0.5 * C0) * g * (1.0 - t * t) * (1.0 + (3.0 * C1) * g2)
    return (dh * u * slope).astype(BF), (dh * gelu).astype(BF), (gelu * u).astype(BF)


def ring_kernel(dy, gate, up, wd, wg, wu,
                dx, h, dyf, dgu0, dgu1, dgu2, dgu3, inb, qb, hold,
                wdv, wgu, dyb, gb, ub, dgu, hb, pv, qs, qin, rin, ob,
                w_s, ld_s, own_s, o_s, ag_r, ag_t, dd_r, dd_t, q_r, q_t, rs_r, rs_t, c_s, hd_s):
    dgus = (dgu0, dgu1, dgu2, dgu3)
    tp = lax.axis_index("tp")
    c = lax.rem(tp, 2)
    z = lax.rem(tp // 2, 4)
    y = tp // 8
    pos = jnp.where(y == 0, z, 7 - z)

    def dev(p, core):
        yy = p // 4
        zz = jnp.where(p < 4, p, 7 - p)
        return (yy * 4 + zz) * 2 + core

    right, left, mate = dev(lax.rem(pos + 1, RING), c), dev(lax.rem(pos + RING - 1, RING), c), dev(pos, 1 - c)
    dirs = (right, left)
    MESH = pl.DeviceIdType.MESH

    bar = pltpu.get_barrier_semaphore()
    for d in (right, left, mate):
        pl.semaphore_signal(bar, inc=1, device_id={"tp": d}, device_id_type=MESH)
    pl.semaphore_wait(bar, 3)

    def remote(src, dst, ss, rs, d):
        return pltpu.make_async_remote_copy(src, dst, ss, rs, device_id={"tp": d}, device_id_type=MESH)

    def start(s, side, core):
        p = lax.rem(pos + RING - s, RING) if side == 0 else lax.rem(pos + s, RING)
        return pl.multiple_of(dev(p, core) * R + side * H, 16)

    def rows(s, side, core):
        return pl.ds(start(s, side, core), H)

    for side in (0, 1):
        half = pl.ds(side * H, H)
        remote(dy.at[half], dyf.at[rows(0, side, c)], ag_t.at[1, side], ag_r.at[1, side], dirs[side]).start()
        remote(dy.at[half], dyf.at[rows(0, side, c)], dd_t.at[0, side], dd_r.at[0, side], mate).start()

    weights = [pltpu.make_async_copy(wd, wdv, w_s.at[0]),
               pltpu.make_async_copy(wg, wgu.at[:, pl.ds(0, F)], w_s.at[1]),
               pltpu.make_async_copy(wu, wgu.at[:, pl.ds(F, F)], w_s.at[2])]
    for w in weights:
        w.start()

    def loads(s, slot):
        core = c if slot == 1 else 1 - c
        out = []
        for side in (0, 1):
            half = pl.ds(side * H, H)
            r = rows(s, side, core)
            out += [pltpu.make_async_copy(dyf.at[r], dyb.at[slot, half], ld_s.at[slot, side, 0]),
                    pltpu.make_async_copy(gate.at[r], gb.at[slot, half], ld_s.at[slot, side, 1]),
                    pltpu.make_async_copy(up.at[r], ub.at[slot, half], ld_s.at[slot, side, 2])]
        return out

    def first_loads():
        out = []
        for side in (0, 1):
            half = pl.ds(side * H, H)
            r = rows(0, side, c)
            out += [pltpu.make_async_copy(dy.at[half], dyb.at[1, half], ld_s.at[1, side, 0]),
                    pltpu.make_async_copy(gate.at[r], gb.at[1, half], ld_s.at[1, side, 1]),
                    pltpu.make_async_copy(up.at[r], ub.at[1, half], ld_s.at[1, side, 2])]
        return out

    own_store = pltpu.make_async_copy(dyb.at[1], dyf.at[pl.ds(pl.multiple_of(dev(pos, c) * R, 16), R)], own_s)

    def stores(s, slot):
        core = c if slot == 1 else 1 - c
        out = []
        k = 0
        for j, (r0, n) in enumerate(PARTS):
            side = 0 if r0 < H else 1
            p = lax.rem(pos + RING - s, RING) if side == 0 else lax.rem(pos + s, RING)
            out.append(pltpu.make_async_copy(dgu.at[pl.ds(r0, n)],
                                             dgus[j].at[pl.ds(pl.multiple_of(dev(p, core) * n, 16), n)], o_s.at[k]))
            k += 1
        for side in (0, 1):
            out.append(pltpu.make_async_copy(hb.at[pl.ds(side * H, H)], h.at[rows(s, side, core)], o_s.at[k]))
            k += 1
        return out

    def dhidden(slot):
        a = dyb[slot]
        for n in range(F // TILE):
            cs = pl.ds(n * TILE, TILE)
            dh = lax.dot_general(a, wdv[n * TILE:(n + 1) * TILE, :], NT, preferred_element_type=F32)
            dg, du, hid = grads(gb[slot, :, cs], ub[slot, :, cs], dh)
            dgu[:, cs] = dg
            dgu[:, pl.ds(F + n * TILE, TILE)] = du
            hb[:, cs] = hid

    def partial_dx(j, store):
        a = dgu[...]
        for n in range(CH // TILE):
            r0 = j * CH + n * TILE
            store(n * TILE, lax.dot_general(a, wgu[r0:r0 + TILE, :], NT, preferred_element_type=F32))

    def q_send(s, j):
        return remote(qs.at[j], qb.at[s, j], q_t.at[j], q_r.at[s, j], mate)

    def rs_send(s, j, side):
        half, cols = pl.ds(side * H, H), pl.ds(j * CH, CH)
        slot = lax.rem(s, 2)
        return remote(ob.at[slot, half, cols], inb.at[s, half, cols], rs_t.at[slot, j, side],
                      rs_r.at[s, j, side], dirs[side])

    def arrived(sem_ref, dst):
        pltpu.make_async_copy(dst, dst, sem_ref).wait()

    def rs_arrived(s, j):
        for side in (0, 1):
            half, cols = pl.ds(side * H, H), pl.ds(j * CH, CH)
            arrived(rs_r.at[s - 1, j, side], inb.at[s - 1, half, cols])

    def in_load(s, j):
        return pltpu.make_async_copy(inb.at[s - 1, :, pl.ds(j * CH, CH)], rin, c_s.at[0])

    def q_load(s, j):
        return pltpu.make_async_copy(qb.at[s, j], qin, c_s.at[1])

    def hold_copy(j):
        return pltpu.make_async_copy(pv.at[:, pl.ds(j * CH, CH)], hold.at[:, pl.ds(j * CH, CH)], hd_s.at[j])

    for cp in first_loads():
        cp.start()
    for side in (0, 1):
        arrived(dd_r.at[0, side], dyf.at[rows(0, side, 1 - c)])
    for cp in loads(0, 0):
        cp.start()
    weights[0].wait()

    def step(s, carry):
        for cp in loads(s, 0):
            cp.wait()

        @pl.when(s > 0)
        def _():
            for cp in stores(s, 1):
                cp.wait()
        dhidden(0)
        for cp in stores(s, 0):
            cp.start()

        @pl.when(s == 0)
        def _():
            weights[1].wait()
            weights[2].wait()
        for j in range(NC):
            @pl.when(s > 0)
            def _():
                q_send(s, j).wait_send()

            def put_q(c0, v):
                qs[j, :, pl.ds(c0, TILE)] = v.astype(BF)
            partial_dx(j, put_q)
            q_send(s, j).start()

        @pl.when(s < RING - 1)
        def _():
            for side in (0, 1):
                r = rows(s + 1, side, c)
                arrived(ag_r.at[s + 1, side], dyf.at[r])

                @pl.when(s < RING - 2)
                def _():
                    remote(dyf.at[r], dyf.at[r], ag_t.at[s + 2, side], ag_r.at[s + 2, side], dirs[side]).start()
                remote(dyf.at[r], dyf.at[r], dd_t.at[s + 1, side], dd_r.at[s + 1, side], mate).start()

        for cp in loads(s, 1):
            cp.wait()

        @pl.when(s == 0)
        def _():
            own_store.start()
        for cp in stores(s, 0):
            cp.wait()
        dhidden(1)
        for cp in stores(s, 1):
            cp.start()

        @pl.when(s == 0)
        def _():
            own_store.wait()

        @pl.when(s < RING - 1)
        def _():
            for cp in loads(s + 1, 1):
                cp.start()

        @pl.when(s == 1)
        def _():
            for j in range(NC):
                hold_copy(j).wait()

        @pl.when(s > 2)
        def _():
            for j in range(NC):
                for side in (0, 1):
                    rs_send(s, j, side).wait_send()

        for j in range(NC):
            arrived(q_r.at[s, j], qb.at[s, j])
            q_load(s, j).start()

            def put_p(c0, v):
                pv[:, pl.ds(j * CH + c0, TILE)] = v
            partial_dx(j, put_p)
            if j == 0:
                @pl.when(s < RING - 1)
                def _():
                    for side in (0, 1):
                        arrived(dd_r.at[s + 1, side], dyf.at[rows(s + 1, side, 1 - c)])
                    for cp in loads(s + 1, 0):
                        cp.start()
            cols = pl.ds(j * CH, CH)

            @pl.when(s > 1)
            def _():
                rs_arrived(s, j)
                in_load(s, j).start()
            q_load(s, j).wait()

            @pl.when(s == 0)
            def _():
                pv[:, cols] = pv[:, cols] + qin[...].astype(F32)
                hold_copy(j).start()

            @pl.when(s == 1)
            def _():
                ob[1, :, cols] = (pv[:, cols] + qin[...].astype(F32)).astype(BF)

            @pl.when(s > 1)
            def _():
                in_load(s, j).wait()
                ob[lax.rem(s, 2), :, cols] = (pv[:, cols] + qin[...].astype(F32) + rin[...].astype(F32)).astype(BF)

            @pl.when(s > 0)
            def _():
                for side in (0, 1):
                    rs_send(s, j, side).start()
        return carry

    lax.fori_loop(0, RING, step, 0)

    for j in range(NC):
        cols = pl.ds(j * CH, CH)
        pltpu.make_async_copy(hold.at[:, cols], pv.at[:, cols], hd_s.at[j]).start()
    for j in range(NC):
        for side in (0, 1):
            rs_send(RING - 2, j, side).wait_send()
    for j in range(NC):
        cols = pl.ds(j * CH, CH)
        rs_arrived(RING, j)
        in_load(RING, j).start()
        pltpu.make_async_copy(hold.at[:, cols], pv.at[:, cols], hd_s.at[j]).wait()
        in_load(RING, j).wait()
        ob[0, :, cols] = (pv[:, cols] + rin[...].astype(F32)).astype(BF)
        pltpu.make_async_copy(ob.at[0, :, cols], dx.at[:, cols], hd_s.at[j]).start()
    for j in range(NC):
        pltpu.make_async_copy(ob.at[0, :, pl.ds(j * CH, CH)], dx.at[:, pl.ds(j * CH, CH)], hd_s.at[j]).wait()
        q_send(0, j).wait_send()
        for side in (0, 1):
            rs_send(RING - 1, j, side).wait_send()
    for cp in stores(RING - 1, 1):
        cp.wait()

    def drain(s, carry):
        for side in (0, 1):
            r = rows(0, side, c)

            @pl.when(s > 0)
            def _():
                remote(dyf.at[r], dyf.at[r], ag_t.at[s, side], ag_r.at[s, side], dirs[side]).wait_send()
            remote(dyf.at[r], dyf.at[r], dd_t.at[s, side], dd_r.at[s, side], mate).wait_send()
        return carry
    lax.fori_loop(0, RING, drain, 0)


def ring_call(dy, gate, up, wd, wg, wu):
    sd = jax.ShapeDtypeStruct
    hbm = pl.BlockSpec(memory_space=pl.ANY)
    outs = [sd((R, D), BF), sd((16 * R, F), BF), sd((16 * R, D), BF)]
    outs += [sd((16 * n, 2 * F), BF) for _, n in PARTS]
    outs += [sd((RING, R, D), BF), sd((RING, NC, R, CH), BF), sd((R, D), F32)]
    dma = pltpu.SemaphoreType.DMA
    return pl.pallas_call(
        ring_kernel,
        out_shape=outs,
        in_specs=[hbm] * 6,
        out_specs=[hbm] * len(outs),
        scratch_shapes=[
            pltpu.VMEM((F, D), BF), pltpu.VMEM((D, 2 * F), BF),
            pltpu.VMEM((2, R, D), BF), pltpu.VMEM((2, R, F), BF), pltpu.VMEM((2, R, F), BF),
            pltpu.VMEM((R, 2 * F), BF), pltpu.VMEM((R, F), BF),
            pltpu.VMEM((R, D), F32), pltpu.VMEM((NC, R, CH), BF),
            pltpu.VMEM((R, CH), BF), pltpu.VMEM((R, CH), BF), pltpu.VMEM((2, R, D), BF),
            dma((3,)), dma((2, 2, 3)), dma, dma((6,)),
            dma((RING, 2)), dma((RING, 2)), dma((RING, 2)), dma((RING, 2)),
            dma((RING, NC)), dma((NC,)), dma((RING, NC, 2)), dma((2, NC, 2)), dma((2,)), dma((NC,)),
        ],
        compiler_params=pltpu.CompilerParams(collective_id=0, has_side_effects=True, vmem_limit_bytes=66_000_000),
        cost_estimate=pl.CostEstimate(flops=3 * 2 * 16 * R * D * F, bytes_accessed=300_000_000, transcendentals=16 * R * F),
        name="ring",
    )(dy, gate, up, wd, wg, wu)


def solution(mesh):
    def body(x, dy, gate, up, w_gate, w_up, w_down):
        outs = ring_call(dy, gate, up, w_down, w_gate, w_up)
        dx, h, dyf = outs[:3]
        dgus = outs[3:7]
        x, dxb = lax.optimization_barrier((x, dx))
        tn = (((0,), (0,)), ((), ()))
        dw_down = lax.dot_general(h, dyf, tn, preferred_element_type=F32).astype(BF)
        acc = None
        for (r0, n), dgu in zip(PARTS, dgus):
            xf = lax.all_gather(x[r0:r0 + n], "tp", axis=0, tiled=True)
            t = lax.dot_general(xf, dgu, tn, preferred_element_type=F32)
            acc = t if acc is None else acc + t
        acc = acc.astype(BF)
        return dxb, acc[:, :F], acc[:, F:], dw_down

    rows, cols = P(("dp", "tp")), P("dp", "tp")
    return jax.shard_map(
        body, mesh=mesh,
        in_specs=(rows, rows, cols, cols, P(None, "tp"), P(None, "tp"), P("tp")),
        out_specs=(rows, cols, cols, P(("dp", "tp"))),
        check_vma=False,
    )
```

```python
import jax
import jax.numpy as jnp
from jax import lax
from jax.experimental import pallas as pl
from jax.experimental.pallas import tpu as pltpu
from jax.sharding import PartitionSpec as P

R, D, F = 352, 3072, 1536
H = R // 2
RING = 8
NC = 2
CH = F
BF, F32 = jnp.bfloat16, jnp.float32
NT = (((1,), (1,)), ((), ()))
C0, C1 = 0.7978845608028654, 0.044715
TILE = 512
KB = 4 * H
SPLIT = ((0, 96), (96, 80))


def grads(g, u, dh):
    g, u = g.astype(F32), u.astype(F32)
    g2 = g * g
    t = jnp.tanh(C0 * (g * (1.0 + C1 * g2)))
    q = 0.5 * (1.0 + t)
    gelu = g * q
    slope = q + (0.5 * C0) * g * (1.0 - t * t) * (1.0 + (3.0 * C1) * g2)
    return (dh * u * slope).astype(BF), (dh * gelu).astype(BF), (gelu * u).astype(BF)


MESH = pl.DeviceIdType.MESH


def place():
    tp = lax.axis_index("tp")
    z = lax.rem(tp // 2, 4)
    return jnp.where(tp < 8, z, 7 - z), lax.rem(tp, 2)


def dev(p, core):
    return (p // 4 * 4 + jnp.where(p < 4, p, 7 - p)) * 2 + core


def start(pos, s, side, core):
    p = lax.rem(pos + RING - s, RING) if side == 0 else lax.rem(pos + s, RING)
    return pl.multiple_of(dev(p, core) * R + side * H, 16)


def greet(devices):
    bar = pltpu.get_barrier_semaphore()
    for d in devices:
        pl.semaphore_signal(bar, inc=1, device_id={"tp": d}, device_id_type=MESH)
    pl.semaphore_wait(bar, len(devices))


def remote(src, dst, ss, rs, d):
    return pltpu.make_async_remote_copy(src, dst, ss, rs, device_id={"tp": d}, device_id_type=MESH)


def arrived(sem, dst):
    pltpu.make_async_copy(dst, dst, sem).wait()


def ring_kernel(dy, gate, up, wd, wg, wu,
                dx, h, dyf, dgo, inb, qb, hold,
                wdv, wgu, dyb, gb, ub, dgu, hb, pv, qs, qin, rin, ob,
                w_s, ld_s, own_s, o_s, ag_r, ag_t, dd_r, dd_t, q_r, q_t, rs_r, rs_t, c_s, hd_s):
    pos, c = place()
    right, left, mate = dev(lax.rem(pos + 1, RING), c), dev(lax.rem(pos + RING - 1, RING), c), dev(pos, 1 - c)
    dirs = (right, left)
    greet((right, left, mate))

    def rows(s, side, core):
        return pl.ds(start(pos, s, side, core), H)

    def slab(s, side, mine):
        return pl.ds(pl.multiple_of(s * KB + (0 if mine else R) + side * H, 16), H)

    def block(s, mine):
        return pl.ds(pl.multiple_of(s * KB + (0 if mine else R), 16), R)

    for side in (0, 1):
        half = pl.ds(side * H, H)
        remote(dy.at[half], dyf.at[slab(1, side, True)], ag_t.at[1, side], ag_r.at[1, side], dirs[side]).start()
        remote(dy.at[half], dyf.at[slab(0, side, False)], dd_t.at[0, side], dd_r.at[0, side], mate).start()

    weights = [pltpu.make_async_copy(wd, wdv, w_s.at[0]),
               pltpu.make_async_copy(wg, wgu.at[:, pl.ds(0, F)], w_s.at[1]),
               pltpu.make_async_copy(wu, wgu.at[:, pl.ds(F, F)], w_s.at[2])]
    for w in weights:
        w.start()

    def loads(s, slot, first=False):
        core = c if slot == 1 else 1 - c
        out = [pltpu.make_async_copy(dy if first else dyf.at[block(s, slot == 1)], dyb.at[slot], ld_s.at[slot, 4])]
        for side in (0, 1):
            half, r = pl.ds(side * H, H), rows(s, side, core)
            out += [pltpu.make_async_copy(gate.at[r], gb.at[slot, half], ld_s.at[slot, 2 * side]),
                    pltpu.make_async_copy(up.at[r], ub.at[slot, half], ld_s.at[slot, 2 * side + 1])]
        return out

    own_store = pltpu.make_async_copy(dyb.at[1], dyf.at[pl.ds(0, R)], own_s)

    def stores(s, slot):
        out = [pltpu.make_async_copy(hb, h.at[block(s, slot == 1)], o_s.at[4])]
        for i, (r0, n) in enumerate(SPLIT):
            for side in (0, 1):
                to = s * KB + 4 * r0 + ((0 if slot == 1 else 2) + side) * n
                out.append(pltpu.make_async_copy(dgu.at[pl.ds(side * H + r0, n)],
                                                 dgo.at[pl.ds(pl.multiple_of(to, 16), n)], o_s.at[2 * i + side]))
        return out

    def dhidden(slot):
        a = dyb[slot]
        for n in range(F // TILE):
            cs = pl.ds(n * TILE, TILE)
            dh = lax.dot_general(a, wdv[n * TILE:(n + 1) * TILE, :], NT, preferred_element_type=F32)
            dg, du, hid = grads(gb[slot, :, cs], ub[slot, :, cs], dh)
            dgu[:, cs] = dg
            dgu[:, pl.ds(F + n * TILE, TILE)] = du
            hb[:, cs] = hid

    def partial_dx(j, store):
        a = dgu[...]
        for n in range(CH // TILE):
            r0 = j * CH + n * TILE
            store(n * TILE, lax.dot_general(a, wgu[r0:r0 + TILE, :], NT, preferred_element_type=F32))

    def q_send(s, j):
        return remote(qs.at[j], qb.at[s, j], q_t.at[j], q_r.at[s, j], mate)

    def rs_send(s, j, side):
        half, cols = pl.ds(side * H, H), pl.ds(j * CH, CH)
        slot = lax.rem(s, 2)
        return remote(ob.at[slot, half, cols], inb.at[s, half, cols], rs_t.at[slot, j, side],
                      rs_r.at[s, j, side], dirs[side])

    def rs_arrived(s, j):
        for side in (0, 1):
            half, cols = pl.ds(side * H, H), pl.ds(j * CH, CH)
            arrived(rs_r.at[s - 1, j, side], inb.at[s - 1, half, cols])

    def in_load(s, j):
        return pltpu.make_async_copy(inb.at[s - 1, :, pl.ds(j * CH, CH)], rin, c_s.at[0])

    def q_load(s, j):
        return pltpu.make_async_copy(qb.at[s, j], qin, c_s.at[1])

    def hold_copy(j):
        return pltpu.make_async_copy(pv.at[:, pl.ds(j * CH, CH)], hold.at[:, pl.ds(j * CH, CH)], hd_s.at[j])

    for cp in loads(0, 1, True):
        cp.start()
    for side in (0, 1):
        arrived(dd_r.at[0, side], dyf.at[slab(0, side, False)])
    for cp in loads(0, 0):
        cp.start()
    weights[0].wait()

    def step(s, carry):
        for cp in loads(s, 0):
            cp.wait()

        @pl.when(s > 0)
        def _():
            for cp in stores(s, 1):
                cp.wait()
        dhidden(0)
        for cp in stores(s, 0):
            cp.start()

        @pl.when(s == 0)
        def _():
            weights[1].wait()
            weights[2].wait()
        for j in range(NC):
            @pl.when(s > 0)
            def _():
                q_send(s, j).wait_send()

            def put_q(c0, v):
                qs[j, :, pl.ds(c0, TILE)] = v.astype(BF)
            partial_dx(j, put_q)
            q_send(s, j).start()

        @pl.when(s < RING - 1)
        def _():
            for side in (0, 1):
                p = dyf.at[slab(s + 1, side, True)]
                arrived(ag_r.at[s + 1, side], p)

                @pl.when(s < RING - 2)
                def _():
                    remote(p, dyf.at[slab(s + 2, side, True)], ag_t.at[s + 2, side], ag_r.at[s + 2, side], dirs[side]).start()
                remote(p, dyf.at[slab(s + 1, side, False)], dd_t.at[s + 1, side], dd_r.at[s + 1, side], mate).start()

        for cp in loads(s, 1):
            cp.wait()

        @pl.when(s == 0)
        def _():
            own_store.start()
        for cp in stores(s, 0):
            cp.wait()
        dhidden(1)
        for cp in stores(s, 1):
            cp.start()

        @pl.when(s == 0)
        def _():
            own_store.wait()

        @pl.when(s < RING - 1)
        def _():
            for cp in loads(s + 1, 1):
                cp.start()

        @pl.when(s == 1)
        def _():
            for j in range(NC):
                hold_copy(j).wait()

        @pl.when(s > 2)
        def _():
            for j in range(NC):
                for side in (0, 1):
                    rs_send(s, j, side).wait_send()

        for j in range(NC):
            arrived(q_r.at[s, j], qb.at[s, j])
            q_load(s, j).start()

            def put_p(c0, v):
                pv[:, pl.ds(j * CH + c0, TILE)] = v
            partial_dx(j, put_p)
            if j == 0:
                @pl.when(s < RING - 1)
                def _():
                    for side in (0, 1):
                        arrived(dd_r.at[s + 1, side], dyf.at[slab(s + 1, side, False)])
                    for cp in loads(s + 1, 0):
                        cp.start()
            cols = pl.ds(j * CH, CH)

            @pl.when(s > 1)
            def _():
                rs_arrived(s, j)
                in_load(s, j).start()
            q_load(s, j).wait()

            @pl.when(s == 0)
            def _():
                pv[:, cols] = pv[:, cols] + qin[...].astype(F32)
                hold_copy(j).start()

            @pl.when(s == 1)
            def _():
                ob[1, :, cols] = (pv[:, cols] + qin[...].astype(F32)).astype(BF)

            @pl.when(s > 1)
            def _():
                in_load(s, j).wait()
                ob[lax.rem(s, 2), :, cols] = (pv[:, cols] + qin[...].astype(F32) + rin[...].astype(F32)).astype(BF)

            @pl.when(s > 0)
            def _():
                for side in (0, 1):
                    rs_send(s, j, side).start()
        return carry

    lax.fori_loop(0, RING, step, 0)

    for j in range(NC):
        cols = pl.ds(j * CH, CH)
        pltpu.make_async_copy(hold.at[:, cols], pv.at[:, cols], hd_s.at[j]).start()
    for j in range(NC):
        for side in (0, 1):
            rs_send(RING - 2, j, side).wait_send()
    for j in range(NC):
        cols = pl.ds(j * CH, CH)
        rs_arrived(RING, j)
        in_load(RING, j).start()
        pltpu.make_async_copy(hold.at[:, cols], pv.at[:, cols], hd_s.at[j]).wait()
        in_load(RING, j).wait()
        ob[0, :, cols] = (pv[:, cols] + rin[...].astype(F32)).astype(BF)
        pltpu.make_async_copy(ob.at[0, :, cols], dx.at[:, cols], hd_s.at[j]).start()
    for j in range(NC):
        pltpu.make_async_copy(ob.at[0, :, pl.ds(j * CH, CH)], dx.at[:, pl.ds(j * CH, CH)], hd_s.at[j]).wait()
        q_send(0, j).wait_send()
        for side in (0, 1):
            rs_send(RING - 1, j, side).wait_send()
    for cp in stores(RING - 1, 1):
        cp.wait()

    def drain(s, carry):
        for side in (0, 1):
            p = dyf.at[slab(0, side, True)]

            @pl.when(s > 0)
            def _():
                remote(p, p, ag_t.at[s, side], ag_r.at[s, side], dirs[side]).wait_send()
            remote(p, p, dd_t.at[s, side], dd_r.at[s, side], mate).wait_send()
        return carry
    lax.fori_loop(0, RING, drain, 0)


def ring_call(dy, gate, up, wd, wg, wu):
    sd = jax.ShapeDtypeStruct
    hbm = pl.BlockSpec(memory_space=pl.ANY)
    outs = [sd((R, D), BF), sd((16 * R, F), BF), sd((16 * R, D), BF)]
    outs += [sd((16 * R, 2 * F), BF)]
    outs += [sd((RING, R, D), BF), sd((RING, NC, R, CH), BF), sd((R, D), F32)]
    dma = pltpu.SemaphoreType.DMA
    return pl.pallas_call(
        ring_kernel,
        out_shape=outs,
        in_specs=[hbm] * 6,
        out_specs=[hbm] * len(outs),
        scratch_shapes=[
            pltpu.VMEM((F, D), BF), pltpu.VMEM((D, 2 * F), BF),
            pltpu.VMEM((2, R, D), BF), pltpu.VMEM((2, R, F), BF), pltpu.VMEM((2, R, F), BF),
            pltpu.VMEM((R, 2 * F), BF), pltpu.VMEM((R, F), BF),
            pltpu.VMEM((R, D), F32), pltpu.VMEM((NC, R, CH), BF),
            pltpu.VMEM((R, CH), BF), pltpu.VMEM((R, CH), BF), pltpu.VMEM((2, R, D), BF),
            dma((3,)), dma((2, 5)), dma, dma((5,)),
            dma((RING, 2)), dma((RING, 2)), dma((RING, 2)), dma((RING, 2)),
            dma((RING, NC)), dma((NC,)), dma((RING, NC, 2)), dma((2, NC, 2)), dma((2,)), dma((NC,)),
        ],
        compiler_params=pltpu.CompilerParams(collective_id=0, has_side_effects=True, vmem_limit_bytes=66_000_000),
        cost_estimate=pl.CostEstimate(flops=3 * 2 * 16 * R * D * F, bytes_accessed=300_000_000, transcendentals=16 * R * F),
        name="ring",
    )(dy, gate, up, wd, wg, wu)


TN = (((0,), (0,)), ((), ()))
NQ = 2 * RING
BLK = 512
NB = 16 * R // BLK
LAST = 2
PACE = 52
CAST = 256
WIDE = 512


def gather_kernel(x, h, dyf, dgu,
                  xf, acc_o, dd_o,
                  acc, xs, ds, st,
                  ag_r, ag_t, dd_r, dd_t, ld_s, st_s, ac_s, own_s):
    pos, c = place()
    right, left, mate = dev(lax.rem(pos + 1, RING), c), dev(lax.rem(pos + RING - 1, RING), c), dev(pos, 1 - c)
    dirs = (right, left)
    greet((right, left, mate))

    def piece(s, i, side, mine):
        r0, n = SPLIT[i]
        return xf.at[pl.ds(pl.multiple_of(s * KB + 4 * r0 + ((0 if mine else 2) + side) * n, 16), n)]

    def pass_on(s, i):
        for side in (0, 1):
            p = piece(s, i, side, True)
            arrived(ag_r.at[2 * s + i, side], p)

            @pl.when(s < RING - 1)
            def _():
                remote(p, piece(s + 1, i, side, True), ag_t.at[2 * s + 2 + i, side], ag_r.at[2 * s + 2 + i, side],
                       dirs[side]).start()
            remote(p, piece(s, i, side, False), dd_t.at[2 * s + i, side], dd_r.at[2 * s + i, side], mate).start()

    def event(q, carry):
        for i in (0, 1):
            @pl.when(lax.rem(q, 2) == i)
            def _():
                pass_on(q // 2, i)
        return carry

    def from_mate(q, carry):
        for i in (0, 1):
            @pl.when(lax.rem(q, 2) == i)
            def _():
                for side in (0, 1):
                    arrived(dd_r.at[q, side], piece(q // 2, i, side, False))
        return carry

    own = pltpu.make_async_copy(x, xs.at[1, pl.ds(0, R)], own_s.at[0])
    own.start()
    for i, (r0, n) in enumerate(SPLIT):
        for side in (0, 1):
            src = x.at[pl.ds(side * H + r0, n)]
            remote(src, piece(1, i, side, True), ag_t.at[2 + i, side], ag_r.at[2 + i, side], dirs[side]).start()
            remote(src, piece(0, i, side, False), dd_t.at[i, side], dd_r.at[i, side], mate).start()

    def down_loads(b, slot):
        r = pl.ds(pl.multiple_of(b * BLK, 16), BLK)
        return [pltpu.make_async_copy(h.at[r], xs.at[slot, :, pl.ds(0, F)], ld_s.at[slot, 0]),
                pltpu.make_async_copy(dyf.at[r], ds.at[slot], ld_s.at[slot, 1])]

    def loads(b, slot):
        r = pl.ds(pl.multiple_of(b * BLK, 16), BLK)
        return [pltpu.make_async_copy(xf.at[r], xs.at[slot], ld_s.at[slot, 2]),
                pltpu.make_async_copy(dgu.at[r], ds.at[slot], ld_s.at[slot, 3])]

    for cp in down_loads(0, 0):
        cp.start()
    own.wait()
    owns = []
    for i, (r0, n) in enumerate(SPLIT):
        for side in (0, 1):
            owns.append(pltpu.make_async_copy(xs.at[1, pl.ds(side * H + r0, n)], piece(0, i, side, True), own_s.at[2 * i + side]))
    for cp in owns:
        cp.start()

    def due(u):
        return 2 + jnp.clip(PACE * (u + 1) - 40, 0, 117 * (NQ - 2)) // 117

    def need(b):
        full = (BLK * (b + 1) - 1) // KB
        return 2 * full + 1 + jnp.where(BLK * (b + 1) - KB * full > 4 * SPLIT[0][1], 1, 0)

    def product(slot, k0, m0, first):
        rows = pl.ds(m0, F)
        a = xs[slot, :, pl.ds(k0, F)]
        for n in range(2 * F // WIDE):
            cols = pl.ds(n * WIDE, WIDE)
            r = lax.dot_general(a, ds[slot, :, cols], TN, preferred_element_type=F32)
            acc[rows, cols] = jnp.where(first, 0.0, acc[rows, cols]) + r

    for cp in owns:
        cp.wait()

    def down(b, carry):
        slot = lax.rem(b, 2)
        for cp in down_loads(b, slot):
            cp.wait()

        @pl.when(b < NB - 1)
        def _():
            for cp in down_loads(b + 1, 1 - slot):
                cp.start()

        @pl.when(b == NB - 1)
        def _():
            lax.fori_loop(0, need(0), from_mate, 0)
            for cp in loads(0, 1 - slot):
                cp.start()
        product(slot, 0, 0, b == 0)
        lax.fori_loop(due(b - 1), due(b), event, 0)
        return carry
    lax.fori_loop(0, NB, down, 0)

    def out_copy(i, slot):
        return pltpu.make_async_copy(st.at[slot], dd_o.at[pl.ds(pl.multiple_of(i * CAST, 16), CAST)], st_s.at[slot])

    def cast(i, carry):
        slot = lax.rem(i, 2)

        @pl.when(i > 1)
        def _():
            out_copy(i - 2, slot).wait()
        st[slot] = acc[pl.ds(pl.multiple_of(i * CAST, 16), CAST), :].astype(BF)
        out_copy(i, slot).start()
        return carry
    lax.fori_loop(0, F // CAST, cast, 0)

    def acc_copy(m):
        rows = pl.ds(pl.multiple_of(m * F, 16), F)
        return pltpu.make_async_copy(acc.at[rows], acc_o.at[rows], ac_s.at[m])

    NG = NB - LAST

    def passed(t):
        n = need(jnp.minimum(t // 2 + 1, NG - 1))
        return jnp.where(t < 0, due(NB - 1), jnp.maximum(due(NB + t), n))

    def unit(t, carry):
        b, m = t // 2, lax.rem(t, 2)
        slot = lax.rem(b + NB, 2)

        @pl.when(m == 0)
        def _():
            for cp in loads(b, slot):
                cp.wait()
        product(slot, pl.multiple_of(m * F, F), pl.multiple_of(m * F, F), b == 0)
        lax.fori_loop(passed(t - 1), passed(t), event, 0)

        @pl.when((m == 0) & (b < NG - 1))
        def _():
            lax.fori_loop(need(b), need(b + 1), from_mate, 0)
            for cp in loads(b + 1, 1 - slot):
                cp.start()

        @pl.when(b == NG - 1)
        def _():
            acc_copy(m).start()
        return carry
    lax.fori_loop(0, 2 * NG, unit, 0)
    lax.fori_loop(passed(2 * NG - 1), NQ, event, 0)
    lax.fori_loop(need(NG - 1), NQ, from_mate, 0)
    for i in (F // CAST - 2, F // CAST - 1):
        out_copy(i, i % 2).wait()
    for m in (0, 1):
        acc_copy(m).wait()

    def drain(q, carry):
        for i in (0, 1):
            @pl.when(lax.rem(q, 2) == i)
            def _():
                for side in (0, 1):
                    p = piece(0, i, side, True)

                    @pl.when(q > 1)
                    def _():
                        remote(p, p, ag_t.at[q, side], ag_r.at[q, side], dirs[side]).wait_send()
                    remote(p, p, dd_t.at[q, side], dd_r.at[q, side], mate).wait_send()
        return carry
    lax.fori_loop(0, NQ, drain, 0)


def gather_call(x, h, dyf, dgu):
    sd = jax.ShapeDtypeStruct
    hbm = pl.BlockSpec(memory_space=pl.ANY)
    outs = [sd((16 * R, D), BF), sd((D, 2 * F), F32), sd((F, D), BF)]
    dma = pltpu.SemaphoreType.DMA
    return pl.pallas_call(
        gather_kernel,
        out_shape=outs,
        in_specs=[hbm] * 4,
        out_specs=[hbm] * 3,
        scratch_shapes=[
            pltpu.VMEM((D, 2 * F), F32), pltpu.VMEM((2, BLK, D), BF), pltpu.VMEM((2, BLK, 2 * F), BF),
            pltpu.VMEM((2, CAST, D), BF),
            dma((NQ, 2)), dma((NQ, 2)), dma((NQ, 2)), dma((NQ, 2)), dma((2, 4)), dma((2,)), dma((2,)), dma((4,)),
        ],
        compiler_params=pltpu.CompilerParams(collective_id=1, has_side_effects=True, vmem_limit_bytes=66_000_000),
        cost_estimate=pl.CostEstimate(flops=3 * 2 * 16 * R * D * F, bytes_accessed=300_000_000, transcendentals=0),
        name="gather",
    )(x, h, dyf, dgu)


ROWS = 512


def last_kernel(xa, xb, da, db, acc, dd, gate, up, down):
    down[...] = dd[...]
    r = lax.dot_general(xa[...], da[...], TN, preferred_element_type=F32)
    r += lax.dot_general(xb[...], db[...], TN, preferred_element_type=F32)
    r += acc[...]
    gate[...] = r[:, :F].astype(BF)
    up[...] = r[:, F:].astype(BF)


def last_call(xf, dgu, acc, dd):
    sd = jax.ShapeDtypeStruct
    n = D // ROWS
    return pl.pallas_call(
        last_kernel,
        grid=(n,),
        out_shape=[sd((D, F), BF), sd((D, F), BF), sd((F, D), BF)],
        in_specs=[pl.BlockSpec((BLK, ROWS), lambda i: (NB - 2, i)), pl.BlockSpec((BLK, ROWS), lambda i: (NB - 1, i)),
                  pl.BlockSpec((BLK, 2 * F), lambda i: (NB - 2, 0)), pl.BlockSpec((BLK, 2 * F), lambda i: (NB - 1, 0)),
                  pl.BlockSpec((ROWS, 2 * F), lambda i: (i, 0)), pl.BlockSpec((F // n, D), lambda i: (i, 0))],
        out_specs=[pl.BlockSpec((ROWS, F), lambda i: (i, 0)), pl.BlockSpec((ROWS, F), lambda i: (i, 0)),
                   pl.BlockSpec((F // n, D), lambda i: (i, 0))],
        compiler_params=pltpu.CompilerParams(dimension_semantics=("arbitrary",), vmem_limit_bytes=66_000_000),
        cost_estimate=pl.CostEstimate(flops=2 * LAST * BLK * D * 2 * F, bytes_accessed=84_000_000, transcendentals=0),
        name="last",
    )(xf, xf, dgu, dgu, acc, dd)


def solution(mesh):
    def body(x, dy, gate, up, w_gate, w_up, w_down):
        dx, h, dyf, dgu = ring_call(dy, gate, up, w_down, w_gate, w_up)[:4]
        xf, acc, dd = gather_call(x, h, dyf, dgu)
        dw_gate, dw_up, dw_down = last_call(xf, dgu, acc, dd)
        return dx, dw_gate, dw_up, dw_down

    rows, cols = P(("dp", "tp")), P("dp", "tp")
    return jax.shard_map(
        body, mesh=mesh,
        in_specs=(rows, rows, cols, cols, P(None, "tp"), P(None, "tp"), P("tp")),
        out_specs=(rows, cols, cols, P(("dp", "tp"))),
        check_vma=False,
    )
```

```python
import jax
import jax.numpy as jnp
from jax import lax
from jax.experimental import pallas as pl
from jax.experimental.pallas import tpu as pltpu
from jax.sharding import PartitionSpec as P

R, D, F = 352, 3072, 1536
H = R // 2
RA = 264
RING = 8
NC = 2
CH = F
BF, F32 = jnp.bfloat16, jnp.float32
NT = (((1,), (1,)), ((), ()))
C0, C1 = 0.7978845608028654, 0.044715
TILE = 512
KB = 4 * H


def grads(g, u, dh):
    g, u = g.astype(F32), u.astype(F32)
    g2 = g * g
    t = jnp.tanh(g * (C0 + (C0 * C1) * g2))
    q = 0.5 + 0.5 * t
    gelu = g * q
    slope = q + gelu * ((1.0 - q) * (2.0 * C0 + (6.0 * C0 * C1) * g2))
    return (dh * (u * slope)).astype(BF), (dh * gelu).astype(BF), (gelu * u).astype(BF)


MESH = pl.DeviceIdType.MESH


def place():
    tp = lax.axis_index("tp")
    y, z, c = tp // 8, lax.rem(tp // 2, 4), lax.rem(tp, 2)
    return y, z, c, jnp.where(y == 0, z, 7 - z)


def dev(p, core):
    return (p // 4 * 4 + jnp.where(p < 4, p, 7 - p)) * 2 + core


def start(pos, s, side, core):
    p = lax.rem(pos + RING - s, RING) if side == 0 else lax.rem(pos + s, RING)
    return pl.multiple_of(dev(p, core) * R + side * H, 16)


def mirrored(z):
    return jnp.where(z < 2, z, 3 - z)


def order(zt, other, zs):
    k = jnp.where(zt < 2, zs, 3 - zs)
    o = jnp.where((mirrored(zt) == 1) & (k < 2), 1 - k, k)
    return 2 * o + other


def greet(y, z, c):
    bar = pltpu.get_barrier_semaphore()

    def hello(d):
        pl.semaphore_signal(bar, inc=1, device_id={"tp": d}, device_id_type=MESH)
    hello((y * 4 + z) * 2 + 1 - c)
    hello(((1 - y) * 4 + z) * 2 + c)

    @pl.when(z < 3)
    def _():
        hello((y * 4 + z + 1) * 2 + c)

    @pl.when(z > 0)
    def _():
        hello((y * 4 + z - 1) * 2 + c)
    pl.semaphore_wait(bar, 2 + jnp.where(z < 3, 1, 0) + jnp.where(z > 0, 1, 0))


def remote(src, dst, ss, rs, d):
    return pltpu.make_async_remote_copy(src, dst, ss, rs, device_id={"tp": d}, device_id_type=MESH)


def arrived(sem, dst):
    pltpu.make_async_copy(dst, dst, sem).wait()


XPARTS = ((0, RA), (RA, R - RA))
PIECE = 88
BOTH = (0, 1)


def xplace(zt, other, zs, part, mine):
    r0, n = XPARTS[part]
    return pl.ds(pl.multiple_of(order(zt, other, zs) * KB + (0 if mine else R) + r0, 8), n)


def back_kernel(x, dy, gate, up, wd, wg, wu,
                h, dyf, dgo, pf, qb, xf,
                wdv, wgu, dyb, gb, ub, dgu, hb, pv, qs,
                w_s, ld_s, own_s, o_s, p_s, ag_r, ag_t, dd_r, dd_t, q_r, q_t, x_r, x_t):
    y, z, c, pos = place()
    right, left, mate = dev(lax.rem(pos + 1, RING), c), dev(lax.rem(pos + RING - 1, RING), c), dev(pos, 1 - c)
    dirs = (right, left)

    def rows(s, side, core):
        return pl.ds(start(pos, s, side, core), H)

    def slab(s, side, part, mine):
        return dyf.at[pl.ds(pl.multiple_of(s * KB + (0 if mine else R) + side * H + part * PIECE, 8), PIECE)]

    def block(s, mine):
        return pl.ds(pl.multiple_of(s * KB + (0 if mine else R), 16), R)

    def ring_copy(src, s, side, part):
        return remote(src, slab(s, side, part, True), ag_t.at[s, side, part], ag_r.at[s, side, part], dirs[side])

    def mate_copy(src, s, side, part):
        return remote(src, slab(s, side, part, False), dd_t.at[s, side, part], dd_r.at[s, side, part], mate)

    weights = [pltpu.make_async_copy(wd, wdv, w_s.at[0]),
               pltpu.make_async_copy(wg, wgu.at[:, pl.ds(0, F)], w_s.at[1]),
               pltpu.make_async_copy(wu, wgu.at[:, pl.ds(F, F)], w_s.at[2])]

    def loads(s, slot, first=False):
        core = c if slot == 1 else 1 - c
        out = [pltpu.make_async_copy(dy if first else dyf.at[block(s, slot == 1)], dyb.at[slot], ld_s.at[slot, 4])]
        for side in BOTH:
            half, r = pl.ds(side * H, H), rows(s, side, core)
            out += [pltpu.make_async_copy(gate.at[r], gb.at[slot, half], ld_s.at[slot, 2 * side]),
                    pltpu.make_async_copy(up.at[r], ub.at[slot, half], ld_s.at[slot, 2 * side + 1])]
        return out

    def stores(s, slot):
        out = [pltpu.make_async_copy(hb, h.at[block(s, slot == 1)], o_s.at[2])]
        for side in BOTH:
            p = lax.rem(pos + RING - s, RING) if side == 0 else lax.rem(pos + s, RING)
            zs = jnp.where(p < 4, p, 7 - p)
            other = jnp.where(p // 4 == y, 0, 1)
            to = order(z, other, zs) * KB + (0 if slot == 1 else R) + side * H
            out.append(pltpu.make_async_copy(dgu.at[pl.ds(side * H, H)], dgo.at[pl.ds(pl.multiple_of(to, 16), H)],
                                             o_s.at[side]))
        return out

    def dhidden(slot):
        a = dyb[slot]
        for n in range(F // TILE):
            cs = pl.ds(n * TILE, TILE)
            dh = lax.dot_general(a, wdv[n * TILE:(n + 1) * TILE, :], NT, preferred_element_type=F32)
            dg, du, hid = grads(gb[slot, :, cs], ub[slot, :, cs], dh)
            dgu[:, cs] = dg
            dgu[:, pl.ds(F + n * TILE, TILE)] = du
            hb[:, cs] = hid

    def partial_dx(j, store):
        a = dgu[...]
        for n in range(CH // TILE):
            r0 = j * CH + n * TILE
            store(r0, lax.dot_general(a, wgu[r0:r0 + TILE, :], NT, preferred_element_type=F32))

    def q_send(s, j):
        return remote(qs.at[j], qb.at[s, :, pl.ds(j * CH, CH)], q_t.at[j], q_r.at[s, j], mate)

    def p_store(s, j):
        cols = pl.ds(j * CH, CH)
        return pltpu.make_async_copy(pv.at[:, cols], pf.at[s, :, cols], p_s.at[j])

    ways = ((z < 3, (y * 4 + z + 1) * 2 + c, 0, z + 1), (z > 0, (y * 4 + z - 1) * 2 + c, 0, z - 1),
            (z >= 0, ((1 - y) * 4 + z) * 2 + c, 1, z))

    def x_send(w, part):
        r0, n = XPARTS[part]
        _, target, other, zt = ways[w]
        return remote(x.at[pl.ds(r0, n)], xf.at[xplace(zt, other, z, part, True)], x_t.at[w, part], x_r.at[w, part], target)

    def x_mate(part):
        r0, n = XPARTS[part]
        return remote(x.at[pl.ds(r0, n)], xf.at[xplace(z, 0, z, part, False)], x_t.at[3, part], x_r.at[3, part], mate)

    weights[0].start()
    for cp in loads(0, 1, True):
        cp.start()
    own_x = [pltpu.make_async_copy(x, dyb.at[0], own_s.at[0]),
             pltpu.make_async_copy(dyb.at[0], xf.at[pl.ds(pl.multiple_of(order(z, 0, z) * KB, 16), R)], own_s.at[0])]
    own_x[0].start()
    own_dy = pltpu.make_async_copy(dyb.at[1], dyf.at[pl.ds(0, R)], own_s.at[1])
    greet(y, z, c)

    for part in BOTH:
        for side in BOTH:
            src = dy.at[pl.ds(side * H + part * PIECE, PIECE)]
            ring_copy(src, 1, side, part).start()
            mate_copy(src, 0, side, part).start()

    weights[0].wait()
    weights[1].start()
    weights[2].start()
    own_x[0].wait()
    own_x[1].start()

    def advance(s, part):
        @pl.when(s < RING - 1)
        def _():
            for side in BOTH:
                p = slab(s + 1, side, part, True)
                arrived(ag_r.at[s + 1, side, part], p)

                @pl.when(s < RING - 2)
                def _():
                    ring_copy(p, s + 2, side, part).start()
                mate_copy(p, s + 1, side, part).start()

    def x_leaves(part):
        for w in range(3):
            @pl.when(ways[w][0])
            def _():
                x_send(w, part).start()
        x_mate(part).start()

    def step(s, carry):
        for cp in loads(s, 1):
            cp.wait()

        @pl.when(s == 0)
        def _():
            own_dy.start()

        @pl.when(s > 0)
        def _():
            for cp in stores(s, 0):
                cp.wait()
            for j in range(NC):
                p_store(s, j).wait()
        dhidden(1)
        for cp in stores(s, 1):
            cp.start()

        @pl.when(s == 0)
        def _():
            own_dy.wait()
            own_x[1].wait()
            weights[1].wait()
            weights[2].wait()

        @pl.when(s < RING - 1)
        def _():
            for cp in loads(s + 1, 1)[1:]:
                cp.start()
        for part in BOTH:
            for side in BOTH:
                arrived(dd_r.at[s, side, part], slab(s, side, part, False))
        for cp in loads(s, 0):
            cp.start()

        def put_p(c0, v):
            pv[:, pl.ds(c0, TILE)] = v
        for j in range(NC):
            partial_dx(j, put_p)
            p_store(s, j).start()
        advance(s, 0)

        for cp in loads(s, 0):
            cp.wait()
        for cp in stores(s, 1):
            cp.wait()

        @pl.when(s > 0)
        def _():
            for j in range(NC):
                q_send(s, j).wait_send()

        def put_q(c0, v):
            qs[c0 // CH, :, pl.ds(c0 % CH, TILE)] = v.astype(BF)
        dhidden(0)
        partial_dx(0, put_q)
        for cp in stores(s, 0):
            cp.start()
        q_send(s, 0).start()
        advance(s, 1)

        @pl.when(s < RING - 1)
        def _():
            loads(s + 1, 1)[0].start()
        for part in BOTH:
            @pl.when(s == XSTEPS[part])
            def _():
                x_leaves(part)
        partial_dx(1, put_q)
        q_send(s, 1).start()
        return carry

    lax.fori_loop(0, RING, step, 0)

    for cp in stores(RING - 1, 0):
        cp.wait()
    for j in range(NC):
        p_store(0, j).wait()
        q_send(0, j).wait_send()
    comes = (z > 0, z < 3, z >= 0)
    for part in BOTH:
        n = XPARTS[part][1]
        for w in range(3):
            @pl.when(comes[w])
            def _():
                arrived(x_r.at[w, part], xf.at[pl.ds(0, n)])

            @pl.when(ways[w][0])
            def _():
                x_send(w, part).wait_send()
        arrived(x_r.at[3, part], xf.at[pl.ds(0, n)])
        x_mate(part).wait_send()

    def drain(s, carry):
        for part in BOTH:
            for side in BOTH:
                p = slab(0, side, part, True)

                @pl.when(s > 0)
                def _():
                    ring_copy(p, s, side, part).wait_send()
                mate_copy(p, s, side, part).wait_send()
        for j in range(NC):
            arrived(q_r.at[s, j], qb.at[0, :, pl.ds(j * CH, CH)])
        return carry
    lax.fori_loop(0, RING, drain, 0)


XSTEPS = (5, 5)


def back_call(x, dy, gate, up, wd, wg, wu):
    sd = jax.ShapeDtypeStruct
    hbm = pl.BlockSpec(memory_space=pl.ANY)
    outs = [sd((16 * R, F), BF), sd((16 * R, D), BF), sd((16 * R, 2 * F), BF), sd((RING, R, D), F32),
            sd((RING, R, D), BF), sd((16 * R, D), BF)]
    dma = pltpu.SemaphoreType.DMA
    return pl.pallas_call(
        back_kernel,
        out_shape=outs,
        in_specs=[hbm] * 7,
        out_specs=[hbm] * len(outs),
        scratch_shapes=[
            pltpu.VMEM((F, D), BF), pltpu.VMEM((D, 2 * F), BF),
            pltpu.VMEM((2, R, D), BF), pltpu.VMEM((2, R, F), BF), pltpu.VMEM((2, R, F), BF),
            pltpu.VMEM((R, 2 * F), BF), pltpu.VMEM((R, F), BF),
            pltpu.VMEM((R, D), F32), pltpu.VMEM((NC, R, CH), BF),
            dma((3,)), dma((2, 5)), dma((2,)), dma((3,)), dma((NC,)),
            dma((RING, 2, 2)), dma((RING, 2, 2)), dma((RING, 2, 2)), dma((RING, 2, 2)),
            dma((RING, NC)), dma((NC,)), dma((4, 2)), dma((4, 2)),
        ],
        compiler_params=pltpu.CompilerParams(collective_id=0, has_side_effects=True, vmem_limit_bytes=66_000_000),
        cost_estimate=pl.CostEstimate(flops=3 * 2 * 16 * R * D * F, bytes_accessed=300_000_000, transcendentals=16 * R * F),
        name="back",
    )(x, dy, gate, up, wd, wg, wu)


TN = (((0,), (0,)), ((), ()))
BLK = 512
NB = 16 * R // BLK
WIDE = 256
CAST = 128
SLOTS = 6
TALL = 768
TALLS = F // TALL
DOWN = NB * TALLS
DOWN_OUT = DOWN + 2
GU = 2 * DOWN
GU_OUT = 4
ENDS = (
    "CJIDSZYTZYZZZyZYUZYZZzZYVZYZZEKmZYZZZLoZYZZFZpZYZZ"
    "QZYuZYZZnZYRZYZZGMvZYZZZNkZYZZZHlZYZZZPiZYwZYZZjZY"
    "xZYZOeZYsZYZZgZYtZYZZhZYqZYZZfZYcZYrZYZZZdZYaZYZbY"
)
INNER = (
    "AELBFKZZZZZJZZZZZZZZZGIZZZZNSZYZZZHTZYZZPMZyZYZZZz"
    "ZYZUZYmZYZZVZOYZZZQZYoZYnZYqZYRZYpZYrZYsZYkZZZYtZY"
    "lZYaZZYwZYiZYcZYxZYjZZZYuZYdZYZZvZYbZYgZYZeZYhZYfY"
)
LETTERS = "ZABCDEFGHIJKLMNOPabcdefghijklmnopqrstuvwxyzQRSTUVY"
SUMS = LETTERS.index("a")
ADD = LETTERS.index("Y")
BASE = 64
PER = 5
ITEMS = len(ENDS)


def packed(work):
    codes = [LETTERS.index(w) for w in work] + [0] * (-len(work) % PER)
    return [sum(code * BASE**j for j, code in enumerate(codes[i:i + PER])) for i in range(0, len(codes), PER)]


def chosen(table, i):
    v = table[0]
    for n, entry in enumerate(table[1:], 1):
        v = jnp.where(i == n, entry, v)
    return v


def reduce_kernel(xin, h, dyf, dgu, pf, qb,
                  xf, lo, hi, iy, dx, og, ou, od,
                  acc, xs, ds, st, pb, ib, ob,
                  x_r, x_t, xd_r, xd_t, lo_r, hi_r, iy_r, ob_s, ld_s, st_s, in_s):
    y, z, c, pos = place()
    end = mirrored(z) == 0
    above, below, across, mate = ((y * 4 + z + 1) * 2 + c, (y * 4 + z - 1) * 2 + c,
                                  ((1 - y) * 4 + z) * 2 + c, (y * 4 + z) * 2 + 1 - c)

    def real(k):
        return jnp.where(z < 2, k, 3 - k)

    def x_sends(other, zs, part):
        src = xf.at[xplace(z, other, zs, part, True)]
        n = other * 4 + zs
        turn = (other == 1) & (zs == z)
        if part == 0:
            go_up, go_down, go_over = (other == 0) & (zs < z), (other == 0) & (zs > z), other == 0
        else:
            go_up, go_down, go_over = (zs < z) | turn, (zs > z) | turn, None
        out = [(go_up & (z < 3), remote(src, xf.at[xplace(z + 1, other, zs, part, True)], x_t.at[0, n, part],
                                        x_r.at[n, part], above)),
               (go_down & (z > 0), remote(src, xf.at[xplace(z - 1, other, zs, part, True)], x_t.at[1, n, part],
                                          x_r.at[n, part], below)),
               (z >= 0, remote(src, xf.at[xplace(z, other, zs, part, False)], xd_t.at[n, part], xd_r.at[n, part], mate))]
        if go_over is not None:
            out.append((go_over, remote(src, xf.at[xplace(z, 1 - other, zs, part, True)], x_t.at[2, n, part],
                                        x_r.at[(1 - other) * 4 + zs, part], across)))
        return out

    def pass_on(other, zs, part):
        first = ((other == 0) & ((zs - z) * (zs - z) == 1)) | ((other == 1) & (zs == z))

        @pl.when(jnp.logical_not(first))
        def _():
            arrived(x_r.at[other * 4 + zs, part], xf.at[xplace(z, other, zs, part, True)])
        for cond, cp in x_sends(other, zs, part):
            @pl.when(cond)
            def _():
                cp.start()

    def slot_from_mate(sl, carry):
        o, other = sl // 2, lax.rem(sl, 2)
        k = jnp.where(end | (o > 1), o, 1 - o)
        for part in BOTH:
            arrived(xd_r.at[other * 4 + real(k), part], xf.at[pl.ds(0, XPARTS[part][1])])
        return carry

    def down_loads(b, slot):
        r = pl.ds(pl.multiple_of(b * BLK, 16), BLK)
        return [pltpu.make_async_copy(h.at[r], xs.at[slot, :, pl.ds(0, F)], ld_s.at[slot, 0]),
                pltpu.make_async_copy(dyf.at[r], ds.at[slot], ld_s.at[slot, 1])]

    def loads(b, slot):
        r = pl.ds(pl.multiple_of(b * BLK, 16), BLK)
        return [pltpu.make_async_copy(xf.at[r], xs.at[slot], ld_s.at[slot, 2]),
                pltpu.make_async_copy(dgu.at[r], ds.at[slot], ld_s.at[slot, 3])]

    def product(slot, m, first):
        rows = pl.ds(pl.multiple_of(m * TALL, TALL), TALL)
        a = xs[slot, :, rows]
        for n in range(2 * F // WIDE):
            cols = pl.ds(n * WIDE, WIDE)
            r = lax.dot_general(a, ds[slot, :, cols], TN, preferred_element_type=F32)
            acc[rows, cols] = jnp.where(first, 0.0, acc[rows, cols]) + r

    def last_slot(b):
        return (BLK * (b + 1) - 1) // KB

    def down_copy(i, slot):
        return [pltpu.make_async_copy(st.at[slot], od.at[pl.ds(pl.multiple_of(i * CAST, 16), CAST)], st_s.at[slot, 0])]

    def weight_copies(i, slot):
        r = pl.ds(pl.multiple_of(i * CAST, 16), CAST)
        return [pltpu.make_async_copy(st.at[slot, :, pl.ds(0, F)], og.at[r], st_s.at[slot, 0]),
                pltpu.make_async_copy(st.at[slot, :, pl.ds(F, F)], ou.at[r], st_s.at[slot, 1])]

    def cast(n, part, parts, copies):
        def one(i, carry):
            slot = lax.rem(i, 2)

            @pl.when(i > 1)
            def _():
                for cp in copies(i, slot):
                    cp.wait()
            st[slot] = acc[pl.ds(pl.multiple_of(i * CAST, 16), CAST), :].astype(BF)
            for cp in copies(i, slot):
                cp.start()
            return carry
        lax.fori_loop(part * (n // parts), (part + 1) * (n // parts), one, 0)

        @pl.when(part == parts - 1)
        def _():
            for i in (n - 2, n - 1):
                for cp in copies(i, i % 2):
                    cp.wait()

    def unit(u):
        v = u - DOWN_OUT
        gu = (v >= 0) & (v < GU)
        b = jnp.where(gu, v // (2 * TALLS), u // TALLS)
        m = jnp.where(gu, lax.rem(v, 2 * TALLS), lax.rem(u, TALLS))
        slot = lax.rem(b + jnp.where(gu, NB, 0), 2)

        @pl.when((u < DOWN) & (m == 0))
        def _():
            for cp in down_loads(b, slot):
                cp.wait()

            @pl.when(b < NB - 1)
            def _():
                for cp in down_loads(b + 1, 1 - slot):
                    cp.start()

            @pl.when(b == NB - 1)
            def _():
                for cp in loads(0, 1 - slot):
                    cp.start()

        @pl.when(gu & (m == 0))
        def _():
            for cp in loads(b, slot):
                cp.wait()

        @pl.when(gu & (m == TALLS) & (b < NB - 1))
        def _():
            lax.fori_loop(last_slot(b) + 1, last_slot(b + 1) + 1, slot_from_mate, 0)
            for cp in loads(b + 1, 1 - slot):
                cp.start()

        @pl.when((u < DOWN) | gu)
        def _():
            product(slot, m, b == 0)

        @pl.when((u >= DOWN) & (v < 0))
        def _():
            cast(F // CAST, u - DOWN, DOWN_OUT - DOWN, down_copy)

        @pl.when(v >= GU)
        def _():
            cast(D // CAST, v - GU, GU_OUT, weight_copies)

    def target(other, zd, piece):
        yd = jnp.where(other == 0, y, 1 - y)
        along = (piece < 2) | (other == 0)
        from_below = along & (z > 0) & (zd >= z)
        from_above = along & (z < 3) & (zd <= z)
        from_over = (other == 0) & ((piece > 1) | (zd == z))
        return yd * 4 + zd, pl.ds(pl.multiple_of(piece * PIECE, 8), PIECE), along, from_below, from_above, from_over

    def sum_loads(other, zd, piece):
        dc, rows, _, from_below, from_above, from_over = target(other, zd, piece)
        pd = jnp.where(dc < 4, zd, 7 - zd)
        s = lax.rem(jnp.where(piece < 2, pos - pd, pd - pos) + RING, RING)
        return [(z >= 0, pltpu.make_async_copy(pf.at[s, rows], pb, in_s.at[0])),
                (z >= 0, pltpu.make_async_copy(qb.at[s, rows], ib.at[0], in_s.at[1])),
                (from_below, pltpu.make_async_copy(lo.at[dc, rows], ib.at[1], in_s.at[2])),
                (from_above, pltpu.make_async_copy(hi.at[dc, rows], ib.at[2], in_s.at[3])),
                (from_over, pltpu.make_async_copy(iy.at[dc, rows], ib.at[3], in_s.at[4]))]

    def sum_load(other, zd, piece):
        dc, rows, _, from_below, from_above, from_over = target(other, zd, piece)
        for cond, sem, buf in ((from_below, lo_r, lo), (from_above, hi_r, hi), (from_over, iy_r, iy)):
            @pl.when(cond)
            def _():
                arrived(sem.at[dc, piece], buf.at[dc, rows])
        for cond, cp in sum_loads(other, zd, piece):
            @pl.when(cond)
            def _():
                cp.start()

    def out_wait(slot):
        pltpu.make_async_copy(ob.at[slot], ob.at[slot], ob_s.at[slot]).wait()

    def sum_send(other, zd, piece, n):
        dc, rows, along, from_below, from_above, from_over = target(other, zd, piece)
        slot = lax.rem(n, SLOTS)
        for cond, cp in sum_loads(other, zd, piece):
            @pl.when(cond)
            def _():
                cp.wait()

        @pl.when(n >= SLOTS)
        def _():
            out_wait(slot)
        for i, cond in ((1, from_below), (2, from_above), (3, from_over)):
            @pl.when(cond)
            def _():
                pb[...] = pb[...] + ib[i].astype(F32)
        ob[slot] = (pb[...] + ib[0].astype(F32)).astype(BF)
        here = along & (zd == z)
        sem = ob_s.at[slot]

        @pl.when(along & (zd > z))
        def _():
            remote(ob.at[slot], lo.at[dc, rows], sem, lo_r.at[dc, piece], above).start()

        @pl.when(along & (zd < z))
        def _():
            remote(ob.at[slot], hi.at[dc, rows], sem, hi_r.at[dc, piece], below).start()

        @pl.when(jnp.logical_not(along) | (here & (other == 1)))
        def _():
            remote(ob.at[slot], iy.at[dc, rows], sem, iy_r.at[dc, piece], across).start()

        @pl.when(here & (other == 0))
        def _():
            pltpu.make_async_copy(ob.at[slot], dx.at[rows], sem).start()

    for cp in down_loads(0, 0):
        cp.start()
    greet(y, z, c)
    tables = packed(ENDS), packed(INNER)

    def item(i, carry):
        u, n, held = carry
        word = jnp.where(end, *(chosen(t, i // PER) for t in tables))
        code = lax.rem(word, BASE)
        for j in range(1, PER):
            code = jnp.where(lax.rem(i, PER) == j, lax.rem(word // BASE**j, BASE), code)

        def piece_of(index):
            return index // 16, real(lax.rem(index // 4, 4)), lax.rem(index, 4)

        @pl.when(code == 0)
        def _():
            unit(u)
        for part in BOTH:
            @pl.when((code > 0) & (code < SUMS) & (lax.rem(code + 1, 2) == part))
            def _():
                pass_on((code - 1) // 8, real(lax.rem((code - 1) // 2, 4)), part)

        @pl.when((code >= SUMS) & (code < ADD))
        def _():
            sum_load(*piece_of(code - SUMS))

        @pl.when(code == ADD)
        def _():
            sum_send(*piece_of(held), n)
        loaded = (code >= SUMS) & (code < ADD)
        return u + jnp.where(code == 0, 1, 0), n + jnp.where(code == ADD, 1, 0), jnp.where(loaded, code - SUMS, held)

    lax.fori_loop(0, ITEMS, item, (jnp.int32(0),) * 3)

    for slot in range(SLOTS):
        out_wait(slot)

    def drain(n, carry):
        other, zs = n // 4, lax.rem(n, 4)

        @pl.when((other == 1) | (zs != z))
        def _():
            for part in BOTH:
                for cond, cp in x_sends(other, zs, part):
                    @pl.when(cond)
                    def _():
                        cp.wait_send()
        return carry
    lax.fori_loop(0, RING, drain, 0)


def reduce_call(xf, h, dyf, dgu, pf, qb):
    sd = jax.ShapeDtypeStruct
    hbm = pl.BlockSpec(memory_space=pl.ANY)
    land = sd((RING, R, D), BF)
    outs = [sd((16 * R, D), BF), land, land, land, sd((R, D), BF), sd((D, F), BF), sd((D, F), BF), sd((F, D), BF)]
    dma = pltpu.SemaphoreType.DMA
    return pl.pallas_call(
        reduce_kernel,
        out_shape=outs,
        in_specs=[hbm] * 6,
        out_specs=[hbm] * len(outs),
        input_output_aliases={0: 0},
        scratch_shapes=[
            pltpu.VMEM((D, 2 * F), F32), pltpu.VMEM((2, BLK, D), BF), pltpu.VMEM((2, BLK, 2 * F), BF),
            pltpu.VMEM((2, CAST, D), BF), pltpu.VMEM((PIECE, D), F32), pltpu.VMEM((4, PIECE, D), BF),
            pltpu.VMEM((SLOTS, PIECE, D), BF),
            dma((RING, 2)), dma((3, RING, 2)), dma((RING, 2)), dma((RING, 2)),
            dma((RING, 4)), dma((RING, 4)), dma((RING, 4)), dma((SLOTS,)), dma((2, 4)), dma((2, 2)), dma((5,)),
        ],
        compiler_params=pltpu.CompilerParams(collective_id=1, has_side_effects=True, vmem_limit_bytes=66_000_000),
        cost_estimate=pl.CostEstimate(flops=3 * 2 * 16 * R * D * F, bytes_accessed=300_000_000, transcendentals=0),
        name="reduce",
    )(xf, h, dyf, dgu, pf, qb)


def copy_kernel(*refs):
    n = len(refs) // 2
    for a, b in zip(refs[:n], refs[n:]):
        b[...] = a[...]


def copy_call(dx, og, ou, od):
    n = 6
    specs = [pl.BlockSpec((R, D // n), lambda i: (0, i)), pl.BlockSpec((D // n, F), lambda i: (i, 0)),
             pl.BlockSpec((D // n, F), lambda i: (i, 0)), pl.BlockSpec((F // n, D), lambda i: (i, 0))]
    return pl.pallas_call(
        copy_kernel,
        grid=(n,),
        out_shape=[jax.ShapeDtypeStruct(a.shape, a.dtype) for a in (dx, og, ou, od)],
        in_specs=specs,
        out_specs=specs,
        compiler_params=pltpu.CompilerParams(dimension_semantics=("arbitrary",), vmem_limit_bytes=66_000_000),
        cost_estimate=pl.CostEstimate(flops=1_000_000, bytes_accessed=61_000_000, transcendentals=0),
        name="copy",
    )(dx, og, ou, od)


def solution(mesh):
    def body(x, dy, gate, up, w_gate, w_up, w_down):
        h, dyf, dgu, pf, qb, xf = back_call(x, dy, gate, up, w_down, w_gate, w_up)
        outs = reduce_call(xf, h, dyf, dgu, pf, qb)
        return tuple(copy_call(*outs[4:]))

    rows, cols = P(("dp", "tp")), P("dp", "tp")
    return jax.shard_map(
        body, mesh=mesh,
        in_specs=(rows, rows, cols, cols, P(None, "tp"), P(None, "tp"), P("tp")),
        out_specs=(rows, cols, cols, P(("dp", "tp"))),
        check_vma=False,
    )
```

```python
import jax
import jax.numpy as jnp
from jax import lax
from jax.experimental import pallas as pl
from jax.experimental.pallas import tpu as pltpu
from jax.sharding import PartitionSpec as P

R, D, F = 352, 3072, 1536
H = R // 2
RA = 264
RING = 8
NC = 2
CH = F
BF, F32 = jnp.bfloat16, jnp.float32
NT = (((1,), (1,)), ((), ()))
C0, C1 = 0.7978845608028654, 0.044715
TILE = 512
KB = 4 * H


def grads(g, u, dh):
    g, u = g.astype(F32), u.astype(F32)
    g2 = g * g
    t = jnp.tanh(g * (C0 + (C0 * C1) * g2))
    q = 0.5 + 0.5 * t
    gelu = g * q
    slope = q + gelu * ((1.0 - q) * (2.0 * C0 + (6.0 * C0 * C1) * g2))
    return (dh * (u * slope)).astype(BF), (dh * gelu).astype(BF), (gelu * u).astype(BF)


MESH = pl.DeviceIdType.MESH


def place():
    tp = lax.axis_index("tp")
    y, z, c = tp // 8, lax.rem(tp // 2, 4), lax.rem(tp, 2)
    return y, z, c, jnp.where(y == 0, z, 7 - z)


def dev(p, core):
    return (p // 4 * 4 + jnp.where(p < 4, p, 7 - p)) * 2 + core


def start(pos, s, side, core):
    p = lax.rem(pos + RING - s, RING) if side == 0 else lax.rem(pos + s, RING)
    return pl.multiple_of(dev(p, core) * R + side * H, 16)


def mirrored(z):
    return jnp.where(z < 2, z, 3 - z)


def order(zt, other, zs):
    k = jnp.where(zt < 2, zs, 3 - zs)
    o = jnp.where((mirrored(zt) == 1) & (k < 2), 1 - k, k)
    return 2 * o + other


def greet(y, z, c):
    bar = pltpu.get_barrier_semaphore()

    def hello(d):
        pl.semaphore_signal(bar, inc=1, device_id={"tp": d}, device_id_type=MESH)
    hello((y * 4 + z) * 2 + 1 - c)
    hello(((1 - y) * 4 + z) * 2 + c)

    @pl.when(z < 3)
    def _():
        hello((y * 4 + z + 1) * 2 + c)

    @pl.when(z > 0)
    def _():
        hello((y * 4 + z - 1) * 2 + c)
    pl.semaphore_wait(bar, 2 + jnp.where(z < 3, 1, 0) + jnp.where(z > 0, 1, 0))


def remote(src, dst, ss, rs, d):
    return pltpu.make_async_remote_copy(src, dst, ss, rs, device_id={"tp": d}, device_id_type=MESH)


def arrived(sem, dst):
    pltpu.make_async_copy(dst, dst, sem).wait()


XPARTS = ((0, RA), (RA, R - RA))
PIECE = 88
BOTH = (0, 1)


def xplace(zt, other, zs, part, mine):
    r0, n = XPARTS[part]
    return pl.ds(pl.multiple_of(order(zt, other, zs) * KB + (0 if mine else R) + r0, 8), n)


def back_kernel(x, dy, gate, up, wd, wg, wu,
                h, dyf, dgo, pf, qb, xf,
                wdv, wgu, dyb, gb, ub, dgu, hb, pv, qs,
                w_s, ld_s, own_s, o_s, p_s, ag_r, ag_t, dd_r, dd_t, q_r, q_t, x_r, x_t):
    y, z, c, pos = place()
    right, left, mate = dev(lax.rem(pos + 1, RING), c), dev(lax.rem(pos + RING - 1, RING), c), dev(pos, 1 - c)
    dirs = (right, left)

    def rows(s, side, core):
        return pl.ds(start(pos, s, side, core), H)

    def slab(s, side, part, mine):
        return dyf.at[pl.ds(pl.multiple_of(s * KB + (0 if mine else R) + side * H + part * PIECE, 8), PIECE)]

    def block(s, mine):
        return pl.ds(pl.multiple_of(s * KB + (0 if mine else R), 16), R)

    def ring_copy(src, s, side, part):
        return remote(src, slab(s, side, part, True), ag_t.at[s, side, part], ag_r.at[s, side, part], dirs[side])

    def mate_copy(src, s, side, part):
        return remote(src, slab(s, side, part, False), dd_t.at[s, side, part], dd_r.at[s, side, part], mate)

    weights = [pltpu.make_async_copy(wd, wdv, w_s.at[0]),
               pltpu.make_async_copy(wg, wgu.at[:, pl.ds(0, F)], w_s.at[1]),
               pltpu.make_async_copy(wu, wgu.at[:, pl.ds(F, F)], w_s.at[2])]

    def loads(s, slot, first=False):
        core = c if slot == 1 else 1 - c
        out = [pltpu.make_async_copy(dy if first else dyf.at[block(s, slot == 1)], dyb.at[slot], ld_s.at[slot, 4])]
        for side in BOTH:
            half, r = pl.ds(side * H, H), rows(s, side, core)
            out += [pltpu.make_async_copy(gate.at[r], gb.at[slot, half], ld_s.at[slot, 2 * side]),
                    pltpu.make_async_copy(up.at[r], ub.at[slot, half], ld_s.at[slot, 2 * side + 1])]
        return out

    def stores(s, slot):
        out = [pltpu.make_async_copy(hb, h.at[block(s, slot == 1)], o_s.at[2])]
        for side in BOTH:
            p = lax.rem(pos + RING - s, RING) if side == 0 else lax.rem(pos + s, RING)
            zs = jnp.where(p < 4, p, 7 - p)
            other = jnp.where(p // 4 == y, 0, 1)
            to = order(z, other, zs) * KB + (0 if slot == 1 else R) + side * H
            out.append(pltpu.make_async_copy(dgu.at[pl.ds(side * H, H)], dgo.at[pl.ds(pl.multiple_of(to, 16), H)],
                                             o_s.at[side]))
        return out

    def dhidden(slot):
        a = dyb[slot]
        for n in range(F // TILE):
            cs = pl.ds(n * TILE, TILE)
            dh = lax.dot_general(a, wdv[n * TILE:(n + 1) * TILE, :], NT, preferred_element_type=F32)
            dg, du, hid = grads(gb[slot, :, cs], ub[slot, :, cs], dh)
            dgu[:, cs] = dg
            dgu[:, pl.ds(F + n * TILE, TILE)] = du
            hb[:, cs] = hid

    def partial_dx(j, store):
        a = dgu[...]
        for n in range(CH // TILE):
            r0 = j * CH + n * TILE
            store(r0, lax.dot_general(a, wgu[r0:r0 + TILE, :], NT, preferred_element_type=F32))

    def q_send(s, j):
        return remote(qs.at[j], qb.at[s, :, pl.ds(j * CH, CH)], q_t.at[j], q_r.at[s, j], mate)

    def p_store(s, j):
        cols = pl.ds(j * CH, CH)
        return pltpu.make_async_copy(pv.at[:, cols], pf.at[s, :, cols], p_s.at[j])

    ways = ((z < 3, (y * 4 + z + 1) * 2 + c, 0, z + 1), (z > 0, (y * 4 + z - 1) * 2 + c, 0, z - 1),
            (z >= 0, ((1 - y) * 4 + z) * 2 + c, 1, z))

    def x_send(w, part):
        r0, n = XPARTS[part]
        _, target, other, zt = ways[w]
        return remote(x.at[pl.ds(r0, n)], xf.at[xplace(zt, other, z, part, True)], x_t.at[w, part], x_r.at[w, part], target)

    def x_mate(part):
        r0, n = XPARTS[part]
        return remote(x.at[pl.ds(r0, n)], xf.at[xplace(z, 0, z, part, False)], x_t.at[3, part], x_r.at[3, part], mate)

    weights[0].start()
    for cp in loads(0, 1, True):
        cp.start()
    own_x = [pltpu.make_async_copy(x, dyb.at[0], own_s.at[0]),
             pltpu.make_async_copy(dyb.at[0], xf.at[pl.ds(pl.multiple_of(order(z, 0, z) * KB, 16), R)], own_s.at[0])]
    own_x[0].start()
    own_dy = pltpu.make_async_copy(dyb.at[1], dyf.at[pl.ds(0, R)], own_s.at[1])
    greet(y, z, c)

    for part in BOTH:
        for side in BOTH:
            src = dy.at[pl.ds(side * H + part * PIECE, PIECE)]
            ring_copy(src, 1, side, part).start()
            mate_copy(src, 0, side, part).start()

    weights[0].wait()
    weights[1].start()
    weights[2].start()
    own_x[0].wait()
    own_x[1].start()

    def advance(s, part):
        @pl.when(s < RING - 1)
        def _():
            for side in BOTH:
                p = slab(s + 1, side, part, True)
                arrived(ag_r.at[s + 1, side, part], p)

                @pl.when(s < RING - 2)
                def _():
                    ring_copy(p, s + 2, side, part).start()
                mate_copy(p, s + 1, side, part).start()

    def x_leaves(part):
        for w in range(3):
            @pl.when(ways[w][0])
            def _():
                x_send(w, part).start()
        x_mate(part).start()

    def step(s, carry):
        for cp in loads(s, 1):
            cp.wait()

        @pl.when(s == 0)
        def _():
            own_dy.start()

        @pl.when(s > 0)
        def _():
            for cp in stores(s, 0):
                cp.wait()
            for j in range(NC):
                p_store(s, j).wait()
        dhidden(1)
        for cp in stores(s, 1):
            cp.start()

        @pl.when(s == 0)
        def _():
            own_dy.wait()
            own_x[1].wait()
            weights[1].wait()
            weights[2].wait()

        @pl.when(s < RING - 1)
        def _():
            for cp in loads(s + 1, 1)[1:]:
                cp.start()
        for part in BOTH:
            for side in BOTH:
                arrived(dd_r.at[s, side, part], slab(s, side, part, False))
        for cp in loads(s, 0):
            cp.start()

        def put_p(c0, v):
            pv[:, pl.ds(c0, TILE)] = v
        for j in range(NC):
            partial_dx(j, put_p)
            p_store(s, j).start()
        advance(s, 0)

        for cp in loads(s, 0):
            cp.wait()
        for cp in stores(s, 1):
            cp.wait()

        @pl.when(s > 0)
        def _():
            for j in range(NC):
                q_send(s, j).wait_send()

        def put_q(c0, v):
            qs[c0 // CH, :, pl.ds(c0 % CH, TILE)] = v.astype(BF)
        dhidden(0)
        partial_dx(0, put_q)
        for cp in stores(s, 0):
            cp.start()
        q_send(s, 0).start()
        advance(s, 1)

        @pl.when(s < RING - 1)
        def _():
            loads(s + 1, 1)[0].start()
        for part in BOTH:
            @pl.when(s == XSTEPS[part])
            def _():
                x_leaves(part)
        partial_dx(1, put_q)
        q_send(s, 1).start()
        return carry

    lax.fori_loop(0, RING, step, 0)

    for cp in stores(RING - 1, 0):
        cp.wait()
    for j in range(NC):
        p_store(0, j).wait()
        q_send(0, j).wait_send()
    comes = (z > 0, z < 3, z >= 0)
    for part in BOTH:
        n = XPARTS[part][1]
        for w in range(3):
            @pl.when(comes[w])
            def _():
                arrived(x_r.at[w, part], xf.at[pl.ds(0, n)])

            @pl.when(ways[w][0])
            def _():
                x_send(w, part).wait_send()
        arrived(x_r.at[3, part], xf.at[pl.ds(0, n)])
        x_mate(part).wait_send()

    def drain(s, carry):
        for part in BOTH:
            for side in BOTH:
                p = slab(0, side, part, True)

                @pl.when(s > 0)
                def _():
                    ring_copy(p, s, side, part).wait_send()
                mate_copy(p, s, side, part).wait_send()
        for j in range(NC):
            arrived(q_r.at[s, j], qb.at[0, :, pl.ds(j * CH, CH)])
        return carry
    lax.fori_loop(0, RING, drain, 0)


XSTEPS = (5, 5)


def back_call(x, dy, gate, up, wd, wg, wu):
    sd = jax.ShapeDtypeStruct
    hbm = pl.BlockSpec(memory_space=pl.ANY)
    outs = [sd((16 * R, F), BF), sd((16 * R, D), BF), sd((16 * R, 2 * F), BF), sd((RING, R, D), F32),
            sd((RING, R, D), BF), sd((16 * R, D), BF)]
    dma = pltpu.SemaphoreType.DMA
    return pl.pallas_call(
        back_kernel,
        out_shape=outs,
        in_specs=[hbm] * 7,
        out_specs=[hbm] * len(outs),
        scratch_shapes=[
            pltpu.VMEM((F, D), BF), pltpu.VMEM((D, 2 * F), BF),
            pltpu.VMEM((2, R, D), BF), pltpu.VMEM((2, R, F), BF), pltpu.VMEM((2, R, F), BF),
            pltpu.VMEM((R, 2 * F), BF), pltpu.VMEM((R, F), BF),
            pltpu.VMEM((R, D), F32), pltpu.VMEM((NC, R, CH), BF),
            dma((3,)), dma((2, 5)), dma((2,)), dma((3,)), dma((NC,)),
            dma((RING, 2, 2)), dma((RING, 2, 2)), dma((RING, 2, 2)), dma((RING, 2, 2)),
            dma((RING, NC)), dma((NC,)), dma((4, 2)), dma((4, 2)),
        ],
        compiler_params=pltpu.CompilerParams(collective_id=0, has_side_effects=True, vmem_limit_bytes=66_000_000),
        cost_estimate=pl.CostEstimate(flops=3 * 2 * 16 * R * D * F, bytes_accessed=300_000_000, transcendentals=16 * R * F),
        name="back",
    )(x, dy, gate, up, wd, wg, wu)


TN = (((0,), (0,)), ((), ()))
BLK = 512
NB = 16 * R // BLK
WIDE = 256
CAST = 128
SLOTS = 6
TALL = 768
TALLS = F // TALL
DOWN = NB * TALLS
DOWN_OUT = DOWN + 2
GU = 2 * DOWN
GU_OUT = 4
ENDS = "".join((
    "CJIDSZYTZYZZZyZYUZYZZzZYVZYZZEKmZYZZZLoZYZZFZpZYZZ",
    "QZYuZYZZnZYRZYZZGMvZYZZZNkZYZZZHlZYZZZPiZYwZYZZjZY",
    "xZYZOeZYsZYZZgZYtZYZZhZYqZYZZfZYcZYrZYZZZdZYaZYZbY",
))
INNER = "".join((
    "AELBFKZZZZZJZZZZZZZZZGIZZZZNSZYZZZHTZYZZPMZyZYZZZz",
    "ZYZUZYmZYZZVZOYZZZQZYoZYnZYqZYRZYpZYrZYsZYkZZZYtZY",
    "lZYaZZYwZYiZYcZYxZYjZZZYuZYdZYZZvZYbZYgZYZeZYhZYfY",
))
LETTERS = "ZABCDEFGHIJKLMNOPabcdefghijklmnopqrstuvwxyzQRSTUVY"
SUMS = LETTERS.index("a")
ADD = LETTERS.index("Y")
BASE = 64
PER = 5
ITEMS = len(ENDS)


def packed(work):
    codes = [LETTERS.index(w) for w in work] + [0] * (-len(work) % PER)
    return [sum(code * BASE**j for j, code in enumerate(codes[i:i + PER])) for i in range(0, len(codes), PER)]


def chosen(table, i):
    v = table[0]
    for n, entry in enumerate(table[1:], 1):
        v = jnp.where(i == n, entry, v)
    return v


def reduce_kernel(xin, h, dyf, dgu, pf, qb,
                  xf, lo, hi, iy, dx, og, ou, od,
                  acc, xs, ds, st, pb, ib, ob,
                  x_r, x_t, xd_r, xd_t, lo_r, hi_r, iy_r, ob_s, ld_s, st_s, in_s):
    y, z, c, pos = place()
    end = mirrored(z) == 0
    above, below, across, mate = ((y * 4 + z + 1) * 2 + c, (y * 4 + z - 1) * 2 + c,
                                  ((1 - y) * 4 + z) * 2 + c, (y * 4 + z) * 2 + 1 - c)

    def real(k):
        return jnp.where(z < 2, k, 3 - k)

    def x_sends(other, zs, part):
        src = xf.at[xplace(z, other, zs, part, True)]
        n = other * 4 + zs
        turn = (other == 1) & (zs == z)
        if part == 0:
            go_up, go_down, go_over = (other == 0) & (zs < z), (other == 0) & (zs > z), other == 0
        else:
            go_up, go_down, go_over = (zs < z) | turn, (zs > z) | turn, None
        out = [(go_up & (z < 3), remote(src, xf.at[xplace(z + 1, other, zs, part, True)], x_t.at[0, n, part],
                                        x_r.at[n, part], above)),
               (go_down & (z > 0), remote(src, xf.at[xplace(z - 1, other, zs, part, True)], x_t.at[1, n, part],
                                          x_r.at[n, part], below)),
               (z >= 0, remote(src, xf.at[xplace(z, other, zs, part, False)], xd_t.at[n, part], xd_r.at[n, part], mate))]
        if go_over is not None:
            out.append((go_over, remote(src, xf.at[xplace(z, 1 - other, zs, part, True)], x_t.at[2, n, part],
                                        x_r.at[(1 - other) * 4 + zs, part], across)))
        return out

    def pass_on(other, zs, part):
        first = ((other == 0) & ((zs - z) * (zs - z) == 1)) | ((other == 1) & (zs == z))

        @pl.when(jnp.logical_not(first))
        def _():
            arrived(x_r.at[other * 4 + zs, part], xf.at[xplace(z, other, zs, part, True)])
        for cond, cp in x_sends(other, zs, part):
            @pl.when(cond)
            def _():
                cp.start()

    def slot_from_mate(sl, carry):
        o, other = sl // 2, lax.rem(sl, 2)
        k = jnp.where(end | (o > 1), o, 1 - o)
        for part in BOTH:
            arrived(xd_r.at[other * 4 + real(k), part], xf.at[pl.ds(0, XPARTS[part][1])])
        return carry

    def down_loads(b, slot):
        r = pl.ds(pl.multiple_of(b * BLK, 16), BLK)
        return [pltpu.make_async_copy(h.at[r], xs.at[slot, :, pl.ds(0, F)], ld_s.at[slot, 0]),
                pltpu.make_async_copy(dyf.at[r], ds.at[slot], ld_s.at[slot, 1])]

    def loads(b, slot):
        r = pl.ds(pl.multiple_of(b * BLK, 16), BLK)
        return [pltpu.make_async_copy(xf.at[r], xs.at[slot], ld_s.at[slot, 2]),
                pltpu.make_async_copy(dgu.at[r], ds.at[slot], ld_s.at[slot, 3])]

    def product(slot, m, first):
        rows = pl.ds(pl.multiple_of(m * TALL, TALL), TALL)
        a = xs[slot, :, rows]
        for n in range(2 * F // WIDE):
            cols = pl.ds(n * WIDE, WIDE)
            r = lax.dot_general(a, ds[slot, :, cols], TN, preferred_element_type=F32)
            acc[rows, cols] = jnp.where(first, 0.0, acc[rows, cols]) + r

    def last_slot(b):
        return (BLK * (b + 1) - 1) // KB

    def down_copy(i, slot):
        return [pltpu.make_async_copy(st.at[slot], od.at[pl.ds(pl.multiple_of(i * CAST, 16), CAST)], st_s.at[slot, 0])]

    def weight_copies(i, slot):
        r = pl.ds(pl.multiple_of(i * CAST, 16), CAST)
        return [pltpu.make_async_copy(st.at[slot, :, pl.ds(0, F)], og.at[r], st_s.at[slot, 0]),
                pltpu.make_async_copy(st.at[slot, :, pl.ds(F, F)], ou.at[r], st_s.at[slot, 1])]

    def cast(n, part, parts, copies):
        def one(i, carry):
            slot = lax.rem(i, 2)

            @pl.when(i > 1)
            def _():
                for cp in copies(i, slot):
                    cp.wait()
            st[slot] = acc[pl.ds(pl.multiple_of(i * CAST, 16), CAST), :].astype(BF)
            for cp in copies(i, slot):
                cp.start()
            return carry
        lax.fori_loop(part * (n // parts), (part + 1) * (n // parts), one, 0)

        @pl.when(part == parts - 1)
        def _():
            for i in (n - 2, n - 1):
                for cp in copies(i, i % 2):
                    cp.wait()

    def unit(u):
        v = u - DOWN_OUT
        gu = (v >= 0) & (v < GU)
        b = jnp.where(gu, v // (2 * TALLS), u // TALLS)
        m = jnp.where(gu, lax.rem(v, 2 * TALLS), lax.rem(u, TALLS))
        slot = lax.rem(b + jnp.where(gu, NB, 0), 2)

        @pl.when((u < DOWN) & (m == 0))
        def _():
            for cp in down_loads(b, slot):
                cp.wait()

            @pl.when(b < NB - 1)
            def _():
                for cp in down_loads(b + 1, 1 - slot):
                    cp.start()

            @pl.when(b == NB - 1)
            def _():
                for cp in loads(0, 1 - slot):
                    cp.start()

        @pl.when(gu & (m == 0))
        def _():
            for cp in loads(b, slot):
                cp.wait()

        @pl.when(gu & (m == TALLS) & (b < NB - 1))
        def _():
            lax.fori_loop(last_slot(b) + 1, last_slot(b + 1) + 1, slot_from_mate, 0)
            for cp in loads(b + 1, 1 - slot):
                cp.start()

        @pl.when((u < DOWN) | gu)
        def _():
            product(slot, m, b == 0)

        @pl.when((u >= DOWN) & (v < 0))
        def _():
            cast(F // CAST, u - DOWN, DOWN_OUT - DOWN, down_copy)

        @pl.when(v >= GU)
        def _():
            cast(D // CAST, v - GU, GU_OUT, weight_copies)

    def target(other, zd, piece):
        yd = jnp.where(other == 0, y, 1 - y)
        along = (piece < 2) | (other == 0)
        from_below = along & (z > 0) & (zd >= z)
        from_above = along & (z < 3) & (zd <= z)
        from_over = (other == 0) & ((piece > 1) | (zd == z))
        return yd * 4 + zd, pl.ds(pl.multiple_of(piece * PIECE, 8), PIECE), along, from_below, from_above, from_over

    def sum_loads(other, zd, piece):
        dc, rows, _, from_below, from_above, from_over = target(other, zd, piece)
        pd = jnp.where(dc < 4, zd, 7 - zd)
        s = lax.rem(jnp.where(piece < 2, pos - pd, pd - pos) + RING, RING)
        return [(z >= 0, pltpu.make_async_copy(pf.at[s, rows], pb, in_s.at[0])),
                (z >= 0, pltpu.make_async_copy(qb.at[s, rows], ib.at[0], in_s.at[1])),
                (from_below, pltpu.make_async_copy(lo.at[dc, rows], ib.at[1], in_s.at[2])),
                (from_above, pltpu.make_async_copy(hi.at[dc, rows], ib.at[2], in_s.at[3])),
                (from_over, pltpu.make_async_copy(iy.at[dc, rows], ib.at[3], in_s.at[4]))]

    def sum_load(other, zd, piece):
        dc, rows, _, from_below, from_above, from_over = target(other, zd, piece)
        for cond, sem, buf in ((from_below, lo_r, lo), (from_above, hi_r, hi), (from_over, iy_r, iy)):
            @pl.when(cond)
            def _():
                arrived(sem.at[dc, piece], buf.at[dc, rows])
        for cond, cp in sum_loads(other, zd, piece):
            @pl.when(cond)
            def _():
                cp.start()

    def out_wait(slot):
        pltpu.make_async_copy(ob.at[slot], ob.at[slot], ob_s.at[slot]).wait()

    def sum_send(other, zd, piece, n):
        dc, rows, along, from_below, from_above, from_over = target(other, zd, piece)
        slot = lax.rem(n, SLOTS)
        for cond, cp in sum_loads(other, zd, piece):
            @pl.when(cond)
            def _():
                cp.wait()

        @pl.when(n >= SLOTS)
        def _():
            out_wait(slot)
        for i, cond in ((1, from_below), (2, from_above), (3, from_over)):
            @pl.when(cond)
            def _():
                pb[...] = pb[...] + ib[i].astype(F32)
        ob[slot] = (pb[...] + ib[0].astype(F32)).astype(BF)
        here = along & (zd == z)
        sem = ob_s.at[slot]

        @pl.when(along & (zd > z))
        def _():
            remote(ob.at[slot], lo.at[dc, rows], sem, lo_r.at[dc, piece], above).start()

        @pl.when(along & (zd < z))
        def _():
            remote(ob.at[slot], hi.at[dc, rows], sem, hi_r.at[dc, piece], below).start()

        @pl.when(jnp.logical_not(along) | (here & (other == 1)))
        def _():
            remote(ob.at[slot], iy.at[dc, rows], sem, iy_r.at[dc, piece], across).start()

        @pl.when(here & (other == 0))
        def _():
            pltpu.make_async_copy(ob.at[slot], dx.at[rows], sem).start()

    for cp in down_loads(0, 0):
        cp.start()
    greet(y, z, c)
    tables = packed(ENDS), packed(INNER)

    def item(i, carry):
        u, n, held = carry
        word = jnp.where(end, *(chosen(t, i // PER) for t in tables))
        code = lax.rem(word, BASE)
        for j in range(1, PER):
            code = jnp.where(lax.rem(i, PER) == j, lax.rem(word // BASE**j, BASE), code)

        def piece_of(index):
            return index // 16, real(lax.rem(index // 4, 4)), lax.rem(index, 4)

        @pl.when(code == 0)
        def _():
            unit(u)
        for part in BOTH:
            @pl.when((code > 0) & (code < SUMS) & (lax.rem(code + 1, 2) == part))
            def _():
                pass_on((code - 1) // 8, real(lax.rem((code - 1) // 2, 4)), part)

        @pl.when((code >= SUMS) & (code < ADD))
        def _():
            sum_load(*piece_of(code - SUMS))

        @pl.when(code == ADD)
        def _():
            sum_send(*piece_of(held), n)
        loaded = (code >= SUMS) & (code < ADD)
        return u + jnp.where(code == 0, 1, 0), n + jnp.where(code == ADD, 1, 0), jnp.where(loaded, code - SUMS, held)

    lax.fori_loop(0, ITEMS, item, (jnp.int32(0),) * 3)

    for slot in range(SLOTS):
        out_wait(slot)

    def drain(n, carry):
        other, zs = n // 4, lax.rem(n, 4)

        @pl.when((other == 1) | (zs != z))
        def _():
            for part in BOTH:
                for cond, cp in x_sends(other, zs, part):
                    @pl.when(cond)
                    def _():
                        cp.wait_send()
        return carry
    lax.fori_loop(0, RING, drain, 0)


def reduce_call(xf, h, dyf, dgu, pf, qb):
    sd = jax.ShapeDtypeStruct
    hbm = pl.BlockSpec(memory_space=pl.ANY)
    land = sd((RING, R, D), BF)
    outs = [sd((16 * R, D), BF), land, land, land, sd((R, D), BF), sd((D, F), BF), sd((D, F), BF), sd((F, D), BF)]
    dma = pltpu.SemaphoreType.DMA
    return pl.pallas_call(
        reduce_kernel,
        out_shape=outs,
        in_specs=[hbm] * 6,
        out_specs=[hbm] * len(outs),
        input_output_aliases={0: 0},
        scratch_shapes=[
            pltpu.VMEM((D, 2 * F), F32), pltpu.VMEM((2, BLK, D), BF), pltpu.VMEM((2, BLK, 2 * F), BF),
            pltpu.VMEM((2, CAST, D), BF), pltpu.VMEM((PIECE, D), F32), pltpu.VMEM((4, PIECE, D), BF),
            pltpu.VMEM((SLOTS, PIECE, D), BF),
            dma((RING, 2)), dma((3, RING, 2)), dma((RING, 2)), dma((RING, 2)),
            dma((RING, 4)), dma((RING, 4)), dma((RING, 4)), dma((SLOTS,)), dma((2, 4)), dma((2, 2)), dma((5,)),
        ],
        compiler_params=pltpu.CompilerParams(collective_id=1, has_side_effects=True, vmem_limit_bytes=66_000_000),
        cost_estimate=pl.CostEstimate(flops=3 * 2 * 16 * R * D * F, bytes_accessed=300_000_000, transcendentals=0),
        name="reduce",
    )(xf, h, dyf, dgu, pf, qb)


def copy_kernel(*refs):
    n = len(refs) // 2
    for a, b in zip(refs[:n], refs[n:]):
        b[...] = a[...]


COPIES = 6


def copy_call(dx, og, ou, od):
    n = COPIES
    specs = [pl.BlockSpec((R, D // n), lambda i: (0, i)), pl.BlockSpec((D // n, F), lambda i: (i, 0)),
             pl.BlockSpec((D // n, F), lambda i: (i, 0)), pl.BlockSpec((F // n, D), lambda i: (i, 0))]
    return pl.pallas_call(
        copy_kernel,
        grid=(n,),
        out_shape=[jax.ShapeDtypeStruct(a.shape, a.dtype) for a in (dx, og, ou, od)],
        in_specs=specs,
        out_specs=specs,
        compiler_params=pltpu.CompilerParams(dimension_semantics=("arbitrary",), vmem_limit_bytes=66_000_000),
        cost_estimate=pl.CostEstimate(flops=1_000_000, bytes_accessed=61_000_000, transcendentals=0),
        name="copy",
    )(dx, og, ou, od)


def solution(mesh):
    def body(x, dy, gate, up, w_gate, w_up, w_down):
        h, dyf, dgu, pf, qb, xf = back_call(x, dy, gate, up, w_down, w_gate, w_up)
        outs = reduce_call(xf, h, dyf, dgu, pf, qb)
        return tuple(copy_call(*outs[4:]))

    rows, cols = P(("dp", "tp")), P("dp", "tp")
    return jax.shard_map(
        body, mesh=mesh,
        in_specs=(rows, rows, cols, cols, P(None, "tp"), P(None, "tp"), P("tp")),
        out_specs=(rows, cols, cols, P(("dp", "tp"))),
        check_vma=False,
    )
```

```python
import jax
import jax.numpy as jnp
from jax import lax
from jax.experimental import pallas as pl
from jax.experimental.pallas import tpu as pltpu
from jax.sharding import PartitionSpec as P

R, D, F = 352, 3072, 1536
H = R // 2
RING = 8
NC = 2
CH = F
BF, F32 = jnp.bfloat16, jnp.float32
NT = (((1,), (1,)), ((), ()))
C0, C1 = 0.7978845608028654, 0.044715
TILE = 512
KB = 4 * H


def grads(g, u, dh):
    g, u = g.astype(F32), u.astype(F32)
    g2 = g * g
    t = jnp.tanh(g * (C0 + (C0 * C1) * g2))
    q = 0.5 + 0.5 * t
    gelu = g * q
    slope = q + gelu * ((1.0 - q) * (2.0 * C0 + (6.0 * C0 * C1) * g2))
    return (dh * (u * slope)).astype(BF), (dh * gelu).astype(BF), (gelu * u).astype(BF)


MESH = pl.DeviceIdType.MESH


def place():
    tp = lax.axis_index("tp")
    y, z, c = tp // 8, lax.rem(tp // 2, 4), lax.rem(tp, 2)
    return y, z, c, jnp.where(y == 0, z, 7 - z)


def dev(p, core):
    return (p // 4 * 4 + jnp.where(p < 4, p, 7 - p)) * 2 + core


def start(pos, s, side, core):
    p = lax.rem(pos + RING - s, RING) if side == 0 else lax.rem(pos + s, RING)
    return pl.multiple_of(dev(p, core) * R + side * H, 16)


def mirrored(z):
    return jnp.where(z < 2, z, 3 - z)


def order(zt, other, zs):
    k = jnp.where(zt < 2, zs, 3 - zs)
    o = jnp.where((mirrored(zt) == 1) & (k < 2), 1 - k, k)
    return 2 * o + other


def home(zs):
    return jnp.where(zs == 0, 1, jnp.where(zs == 3, 2, zs))


def greet(y, z, c):
    bar = pltpu.get_barrier_semaphore()

    def hello(d):
        pl.semaphore_signal(bar, inc=1, device_id={"tp": d}, device_id_type=MESH)
    hello((y * 4 + z) * 2 + 1 - c)
    hello(((1 - y) * 4 + z) * 2 + c)

    @pl.when(z < 3)
    def _():
        hello((y * 4 + z + 1) * 2 + c)

    @pl.when(z > 0)
    def _():
        hello((y * 4 + z - 1) * 2 + c)
    pl.semaphore_wait(bar, 2 + jnp.where(z < 3, 1, 0) + jnp.where(z > 0, 1, 0))


def remote(src, dst, ss, rs, d):
    return pltpu.make_async_remote_copy(src, dst, ss, rs, device_id={"tp": d}, device_id_type=MESH)


def arrived(sem, dst):
    pltpu.make_async_copy(dst, dst, sem).wait()


XPARTS = ((0, 176), (176, 88), (264, 88))
PARTS = (0, 1, 2)
CROSS = 2
PIECE = 88
BOTH = (0, 1)


def xplace(zt, other, zs, part, mine):
    r0, n = XPARTS[part]
    return pl.ds(pl.multiple_of(order(zt, other, zs) * KB + (0 if mine else R) + r0, 8), n)


def back_kernel(x, dy, gate, up, wd, wg, wu,
                h, dyf, dgo, pf, qb, xf,
                wdv, wgu, dyb, gb, ub, dgu, hb, pv, qs,
                w_s, ld_s, own_s, o_s, p_s, ag_r, ag_t, dd_r, dd_t, q_r, q_t, x_r, x_t):
    y, z, c, pos = place()
    right, left, mate = dev(lax.rem(pos + 1, RING), c), dev(lax.rem(pos + RING - 1, RING), c), dev(pos, 1 - c)
    dirs = (right, left)

    def rows(s, side, core):
        return pl.ds(start(pos, s, side, core), H)

    def slab(s, side, part, mine):
        return dyf.at[pl.ds(pl.multiple_of(s * KB + (0 if mine else R) + side * H + part * PIECE, 8), PIECE)]

    def block(s, mine):
        return pl.ds(pl.multiple_of(s * KB + (0 if mine else R), 16), R)

    def ring_copy(src, s, side, part):
        return remote(src, slab(s, side, part, True), ag_t.at[s, side, part], ag_r.at[s, side, part], dirs[side])

    def mate_copy(src, s, side, part):
        return remote(src, slab(s, side, part, False), dd_t.at[s, side, part], dd_r.at[s, side, part], mate)

    weights = [pltpu.make_async_copy(wd, wdv, w_s.at[0]),
               pltpu.make_async_copy(wg, wgu.at[:, pl.ds(0, F)], w_s.at[1]),
               pltpu.make_async_copy(wu, wgu.at[:, pl.ds(F, F)], w_s.at[2])]

    def loads(s, slot, first=False):
        core = c if slot == 1 else 1 - c
        out = [pltpu.make_async_copy(dy if first else dyf.at[block(s, slot == 1)], dyb.at[slot], ld_s.at[slot, 4])]
        for side in BOTH:
            half, r = pl.ds(side * H, H), rows(s, side, core)
            out += [pltpu.make_async_copy(gate.at[r], gb.at[slot, half], ld_s.at[slot, 2 * side]),
                    pltpu.make_async_copy(up.at[r], ub.at[slot, half], ld_s.at[slot, 2 * side + 1])]
        return out

    def stores(s, slot):
        out = [pltpu.make_async_copy(hb, h.at[block(s, slot == 1)], o_s.at[2])]
        for side in BOTH:
            p = lax.rem(pos + RING - s, RING) if side == 0 else lax.rem(pos + s, RING)
            zs = jnp.where(p < 4, p, 7 - p)
            other = jnp.where(p // 4 == y, 0, 1)
            to = order(z, other, zs) * KB + (0 if slot == 1 else R) + side * H
            out.append(pltpu.make_async_copy(dgu.at[pl.ds(side * H, H)], dgo.at[pl.ds(pl.multiple_of(to, 16), H)],
                                             o_s.at[side]))
        return out

    def dhidden(slot):
        a = dyb[slot]
        for n in range(F // TILE):
            cs = pl.ds(n * TILE, TILE)
            dh = lax.dot_general(a, wdv[n * TILE:(n + 1) * TILE, :], NT, preferred_element_type=F32)
            dg, du, hid = grads(gb[slot, :, cs], ub[slot, :, cs], dh)
            dgu[:, cs] = dg
            dgu[:, pl.ds(F + n * TILE, TILE)] = du
            hb[:, cs] = hid

    def partial_dx(j, store):
        a = dgu[...]
        for n in range(CH // TILE):
            r0 = j * CH + n * TILE
            store(r0, lax.dot_general(a, wgu[r0:r0 + TILE, :], NT, preferred_element_type=F32))

    def q_send(s, j):
        return remote(qs.at[j], qb.at[s, :, pl.ds(j * CH, CH)], q_t.at[j], q_r.at[s, j], mate)

    def p_store(s, j):
        cols = pl.ds(j * CH, CH)
        return pltpu.make_async_copy(pv.at[:, cols], pf.at[s, :, cols], p_s.at[j])

    inner = home(z) == z
    over = ((1 - y) * 4 + z) * 2 + c
    ways = ((z < 3, (y * 4 + z + 1) * 2 + c, 0, z + 1), (z > 0, (y * 4 + z - 1) * 2 + c, 0, z - 1), (z >= 0, over, 1, z))
    comes = (z > 0, z < 3, z >= 0)

    def first_hop(w, part, there):
        if w == 3:
            return z >= 0
        if w == 2:
            return inner if part == CROSS else there[w]
        return there[w] if part != 1 else z < 0

    def x_send(w, part):
        r0, n = XPARTS[part]
        src = x.at[pl.ds(r0, n)]
        if w == 3:
            return remote(src, xf.at[xplace(z, 0, z, part, False)], x_t.at[w, part], x_r.at[w, part], mate)
        _, target, other, zt = ways[w]
        return remote(src, xf.at[xplace(zt, other, z, part, True)], x_t.at[w, part], x_r.at[w, part], target)

    zc = jnp.where(z == 1, 0, 3)
    crossing = remote(xf.at[xplace(z, 0, zc, CROSS, True)], xf.at[xplace(z, 1, zc, CROSS, True)],
                      x_t.at[4, CROSS], x_r.at[4, CROSS], over)

    def x_here(w, part):
        arrived(x_r.at[w, part], xf.at[pl.ds(0, XPARTS[part][1])])

    def cross():
        for w, zi in ((0, 1), (1, 2)):
            @pl.when(z == zi)
            def _():
                x_here(w, CROSS)
                crossing.start()

    weights[0].start()
    for cp in loads(0, 1, True):
        cp.start()
    own_x = [pltpu.make_async_copy(x, dyb.at[0], own_s.at[0]),
             pltpu.make_async_copy(dyb.at[0], xf.at[pl.ds(pl.multiple_of(order(z, 0, z) * KB, 16), R)], own_s.at[0])]
    own_x[0].start()
    own_dy = pltpu.make_async_copy(dyb.at[1], dyf.at[pl.ds(0, R)], own_s.at[1])
    greet(y, z, c)

    for part in BOTH:
        for side in BOTH:
            src = dy.at[pl.ds(side * H + part * PIECE, PIECE)]
            ring_copy(src, 1, side, part).start()
            mate_copy(src, 0, side, part).start()

    weights[0].wait()
    weights[1].start()
    weights[2].start()
    own_x[0].wait()
    own_x[1].start()

    def advance(s, part):
        @pl.when(s < RING - 1)
        def _():
            for side in BOTH:
                p = slab(s + 1, side, part, True)
                arrived(ag_r.at[s + 1, side, part], p)

                @pl.when(s < RING - 2)
                def _():
                    ring_copy(p, s + 2, side, part).start()
                mate_copy(p, s + 1, side, part).start()

    def x_leaves():
        for part in reversed(PARTS):
            for w in range(4):
                @pl.when(first_hop(w, part, [way[0] for way in ways]))
                def _():
                    x_send(w, part).start()

    def step(s, carry):
        for cp in loads(s, 1):
            cp.wait()

        @pl.when(s == 0)
        def _():
            own_dy.start()

        @pl.when(s > 0)
        def _():
            for cp in stores(s, 0):
                cp.wait()
            for j in range(NC):
                p_store(s, j).wait()
        dhidden(1)
        for cp in stores(s, 1):
            cp.start()

        @pl.when(s == 0)
        def _():
            own_dy.wait()
            own_x[1].wait()
            weights[1].wait()
            weights[2].wait()

        @pl.when(s < RING - 1)
        def _():
            for cp in loads(s + 1, 1)[1:]:
                cp.start()
        for part in BOTH:
            for side in BOTH:
                arrived(dd_r.at[s, side, part], slab(s, side, part, False))
        for cp in loads(s, 0):
            cp.start()

        def put_p(c0, v):
            pv[:, pl.ds(c0, TILE)] = v
        for j in range(NC):
            partial_dx(j, put_p)
            p_store(s, j).start()
        advance(s, 0)

        @pl.when(s == RING - 1)
        def _():
            cross()

        for cp in loads(s, 0):
            cp.wait()
        for cp in stores(s, 1):
            cp.wait()

        @pl.when(s > 0)
        def _():
            for j in range(NC):
                q_send(s, j).wait_send()

        def put_q(c0, v):
            qs[c0 // CH, :, pl.ds(c0 % CH, TILE)] = v.astype(BF)
        dhidden(0)
        partial_dx(0, put_q)
        for cp in stores(s, 0):
            cp.start()
        q_send(s, 0).start()
        advance(s, 1)

        @pl.when(s < RING - 1)
        def _():
            loads(s + 1, 1)[0].start()

        @pl.when(s == XSTEP)
        def _():
            x_leaves()
        partial_dx(1, put_q)
        q_send(s, 1).start()
        return carry

    lax.fori_loop(0, RING, step, 0)

    for cp in stores(RING - 1, 0):
        cp.wait()
    for j in range(NC):
        p_store(0, j).wait()
        q_send(0, j).wait_send()
    for part in PARTS:
        for w in range(4):
            took = first_hop(w, part, comes)
            if part == CROSS and w < 2:
                took = took & (z != w + 1)

            @pl.when(took)
            def _():
                x_here(w, part)

            @pl.when(first_hop(w, part, [way[0] for way in ways]))
            def _():
                x_send(w, part).wait_send()

    @pl.when(inner)
    def _():
        x_here(4, CROSS)
        crossing.wait_send()

    def drain(s, carry):
        for part in BOTH:
            for side in BOTH:
                p = slab(0, side, part, True)

                @pl.when(s > 0)
                def _():
                    ring_copy(p, s, side, part).wait_send()
                mate_copy(p, s, side, part).wait_send()
        for j in range(NC):
            arrived(q_r.at[s, j], qb.at[0, :, pl.ds(j * CH, CH)])
        return carry
    lax.fori_loop(0, RING, drain, 0)


XSTEP = 5


def back_call(x, dy, gate, up, wd, wg, wu):
    sd = jax.ShapeDtypeStruct
    hbm = pl.BlockSpec(memory_space=pl.ANY)
    outs = [sd((16 * R, F), BF), sd((16 * R, D), BF), sd((16 * R, 2 * F), BF), sd((RING, R, D), F32),
            sd((RING, R, D), BF), sd((16 * R, D), BF)]
    dma = pltpu.SemaphoreType.DMA
    return pl.pallas_call(
        back_kernel,
        out_shape=outs,
        in_specs=[hbm] * 7,
        out_specs=[hbm] * len(outs),
        scratch_shapes=[
            pltpu.VMEM((F, D), BF), pltpu.VMEM((D, 2 * F), BF),
            pltpu.VMEM((2, R, D), BF), pltpu.VMEM((2, R, F), BF), pltpu.VMEM((2, R, F), BF),
            pltpu.VMEM((R, 2 * F), BF), pltpu.VMEM((R, F), BF),
            pltpu.VMEM((R, D), F32), pltpu.VMEM((NC, R, CH), BF),
            dma((3,)), dma((2, 5)), dma((2,)), dma((3,)), dma((NC,)),
            dma((RING, 2, 2)), dma((RING, 2, 2)), dma((RING, 2, 2)), dma((RING, 2, 2)),
            dma((RING, NC)), dma((NC,)), dma((5, 3)), dma((5, 3)),
        ],
        compiler_params=pltpu.CompilerParams(collective_id=0, has_side_effects=True, vmem_limit_bytes=66_000_000),
        cost_estimate=pl.CostEstimate(flops=3 * 2 * 16 * R * D * F, bytes_accessed=300_000_000, transcendentals=16 * R * F),
        name="back",
    )(x, dy, gate, up, wd, wg, wu)


TN = (((0,), (0,)), ((), ()))
BLK = 512
NB = 16 * R // BLK
WIDE = 256
CAST = 128
SLOTS = 6
TALL = 768
TALLS = F // TALL
DOWN = NB * TALLS
DOWN_OUT = DOWN + 2
GU = 2 * DOWN
GU_OUT = 4
ENDS = "".join((
    "DMFN2ZYyZYZZ4ZEYuZYZZZPmZYZZ0GQZYiZYZZRoZYZZZOeZYZ",
    "ZwZSIY3ZYZ5ZHYkZYZZZgZYZZsZJTYzZYZZZUpZYZZZXvZYZZ1",
    "ZVLYnZYZxZKYjZYZZZlZYZZqZWYcYfYZZtZYhZYZZaZYrZYZZd",
    "ZYZZZbY",
))
INNER = "".join((
    "AGROCIPQZZZZZBHZZZZMZZZZJZZZZUSZZZZXNZZZ2ZLTYZZyZY",
    "4ZKYZZmZYZVZZiZY0ZWYZZ3ZYuZYZZoZYsZYZkZYqZY5ZYeZYz",
    "ZYcZY1ZZYaZYpZYtZYwZYrZYnZYZvZYjZYdZYxZYZlZYbZYgZY",
    "fZYZZhY",
))
LETTERS = "ZABCDEFGHIJKLMNOPQRSTUVWXabcdefghijklmnopqrstuvwxyz012345Y"
SUMS = LETTERS.index("a")
ADD = LETTERS.index("Y")
BASE = 64
PER = 5
ITEMS = len(ENDS)


def packed(work):
    codes = [LETTERS.index(w) for w in work] + [0] * (-len(work) % PER)
    return [sum(code * BASE**j for j, code in enumerate(codes[i:i + PER])) for i in range(0, len(codes), PER)]


def chosen(table, i):
    v = table[0]
    for n, entry in enumerate(table[1:], 1):
        v = jnp.where(i == n, entry, v)
    return v


def reduce_kernel(xin, h, dyf, dgu, pf, qb,
                  xf, lo, hi, iy, dx, og, ou, od,
                  acc, xs, ds, st, pb, ib, ob,
                  x_r, x_t, xd_r, xd_t, lo_r, hi_r, iy_r, ob_s, ld_s, st_s, in_s):
    y, z, c, pos = place()
    end = mirrored(z) == 0
    above, below, across, mate = ((y * 4 + z + 1) * 2 + c, (y * 4 + z - 1) * 2 + c,
                                  ((1 - y) * 4 + z) * 2 + c, (y * 4 + z) * 2 + 1 - c)

    def real(k):
        return jnp.where(z < 2, k, 3 - k)

    def hop_up(other, zs, part):
        src = xf.at[xplace(z, other, zs, part, True)]
        return remote(src, xf.at[xplace(z + 1, other, zs, part, True)], x_t.at[0, other * 4 + zs, part],
                      x_r.at[other * 4 + zs, part], above)

    def hop_down(other, zs, part):
        src = xf.at[xplace(z, other, zs, part, True)]
        return remote(src, xf.at[xplace(z - 1, other, zs, part, True)], x_t.at[1, other * 4 + zs, part],
                      x_r.at[other * 4 + zs, part], below)

    def x_sends(other, zs, part):
        src = xf.at[xplace(z, other, zs, part, True)]
        n = other * 4 + zs
        if part == CROSS:
            root = jnp.where(other == 0, zs, home(zs))
            turn = (other == 1) & (root == z)
            go_up, go_down = (root < z) | turn, (root > z) | turn
        else:
            go_up, go_down = (other == 0) & (zs < z), (other == 0) & (zs > z)
        out = [(go_up & (z < 3), hop_up(other, zs, part)), (go_down & (z > 0), hop_down(other, zs, part)),
               (z >= 0, remote(src, xf.at[xplace(z, other, zs, part, False)], xd_t.at[n, part], xd_r.at[n, part], mate))]
        if part != CROSS:
            out.append((other == 0, remote(src, xf.at[xplace(z, 1 - other, zs, part, True)], x_t.at[2, n, part],
                                           x_r.at[(1 - other) * 4 + zs, part], across)))
        return out

    def pass_on(other, zs, part):
        near = (other == 0) & ((zs - z) * (zs - z) == 1)
        if part == 0:
            first = near | ((other == 1) & (zs == z))
        elif part == 1:
            first = (other == 1) & (zs == z)
        else:
            first = near | ((other == 1) & (home(zs) == z))

        @pl.when(jnp.logical_not(first))
        def _():
            arrived(x_r.at[other * 4 + zs, part], xf.at[xplace(z, other, zs, part, True)])
        for cond, cp in x_sends(other, zs, part):
            @pl.when(cond)
            def _():
                cp.start()

    own_hops = ((z < 3, hop_up(0, z, 1)), (z > 0, hop_down(0, z, 1)))

    def slot_from_mate(sl, carry):
        o, other = sl // 2, lax.rem(sl, 2)
        k = jnp.where(end | (o > 1), o, 1 - o)
        for part in PARTS:
            arrived(xd_r.at[other * 4 + real(k), part], xf.at[pl.ds(0, XPARTS[part][1])])
        return carry

    def down_loads(b, slot):
        r = pl.ds(pl.multiple_of(b * BLK, 16), BLK)
        return [pltpu.make_async_copy(h.at[r], xs.at[slot, :, pl.ds(0, F)], ld_s.at[slot, 0]),
                pltpu.make_async_copy(dyf.at[r], ds.at[slot], ld_s.at[slot, 1])]

    def loads(b, slot):
        r = pl.ds(pl.multiple_of(b * BLK, 16), BLK)
        return [pltpu.make_async_copy(xf.at[r], xs.at[slot], ld_s.at[slot, 2]),
                pltpu.make_async_copy(dgu.at[r], ds.at[slot], ld_s.at[slot, 3])]

    def product(slot, m, first):
        rows = pl.ds(pl.multiple_of(m * TALL, TALL), TALL)
        a = xs[slot, :, rows]
        for n in range(2 * F // WIDE):
            cols = pl.ds(n * WIDE, WIDE)
            r = lax.dot_general(a, ds[slot, :, cols], TN, preferred_element_type=F32)
            acc[rows, cols] = jnp.where(first, 0.0, acc[rows, cols]) + r

    def last_slot(b):
        return (BLK * (b + 1) - 1) // KB

    def down_copy(i, slot):
        return [pltpu.make_async_copy(st.at[slot], od.at[pl.ds(pl.multiple_of(i * CAST, 16), CAST)], st_s.at[slot, 0])]

    def weight_copies(i, slot):
        r = pl.ds(pl.multiple_of(i * CAST, 16), CAST)
        return [pltpu.make_async_copy(st.at[slot, :, pl.ds(0, F)], og.at[r], st_s.at[slot, 0]),
                pltpu.make_async_copy(st.at[slot, :, pl.ds(F, F)], ou.at[r], st_s.at[slot, 1])]

    def cast(n, part, parts, copies):
        def one(i, carry):
            slot = lax.rem(i, 2)

            @pl.when(i > 1)
            def _():
                for cp in copies(i, slot):
                    cp.wait()
            st[slot] = acc[pl.ds(pl.multiple_of(i * CAST, 16), CAST), :].astype(BF)
            for cp in copies(i, slot):
                cp.start()
            return carry
        lax.fori_loop(part * (n // parts), (part + 1) * (n // parts), one, 0)

        @pl.when(part == parts - 1)
        def _():
            for i in (n - 2, n - 1):
                for cp in copies(i, i % 2):
                    cp.wait()

    def unit(u):
        v = u - DOWN_OUT
        gu = (v >= 0) & (v < GU)
        b = jnp.where(gu, v // (2 * TALLS), u // TALLS)
        m = jnp.where(gu, lax.rem(v, 2 * TALLS), lax.rem(u, TALLS))
        slot = lax.rem(b + jnp.where(gu, NB, 0), 2)

        @pl.when((u < DOWN) & (m == 0))
        def _():
            for cp in down_loads(b, slot):
                cp.wait()

            @pl.when(b < NB - 1)
            def _():
                for cp in down_loads(b + 1, 1 - slot):
                    cp.start()

            @pl.when(b == NB - 1)
            def _():
                for cp in loads(0, 1 - slot):
                    cp.start()

        @pl.when(gu & (m == 0))
        def _():
            for cp in loads(b, slot):
                cp.wait()

        @pl.when(gu & (m == TALLS) & (b < NB - 1))
        def _():
            lax.fori_loop(last_slot(b) + 1, last_slot(b + 1) + 1, slot_from_mate, 0)
            for cp in loads(b + 1, 1 - slot):
                cp.start()

        @pl.when((u < DOWN) | gu)
        def _():
            product(slot, m, b == 0)

        @pl.when((u >= DOWN) & (v < 0))
        def _():
            cast(F // CAST, u - DOWN, DOWN_OUT - DOWN, down_copy)

        @pl.when(v >= GU)
        def _():
            cast(D // CAST, v - GU, GU_OUT, weight_copies)

    def target(other, zd, piece):
        yd = jnp.where(other == 0, y, 1 - y)
        along = (piece < 2) | (other == 0)
        from_below = along & (z > 0) & (zd >= z)
        from_above = along & (z < 3) & (zd <= z)
        from_over = (other == 0) & ((piece > 1) | (zd == z))
        return yd * 4 + zd, pl.ds(pl.multiple_of(piece * PIECE, 8), PIECE), along, from_below, from_above, from_over

    def sum_loads(other, zd, piece):
        dc, rows, _, from_below, from_above, from_over = target(other, zd, piece)
        pd = jnp.where(dc < 4, zd, 7 - zd)
        s = lax.rem(jnp.where(piece < 2, pos - pd, pd - pos) + RING, RING)
        return [(z >= 0, pltpu.make_async_copy(pf.at[s, rows], pb, in_s.at[0])),
                (z >= 0, pltpu.make_async_copy(qb.at[s, rows], ib.at[0], in_s.at[1])),
                (from_below, pltpu.make_async_copy(lo.at[dc, rows], ib.at[1], in_s.at[2])),
                (from_above, pltpu.make_async_copy(hi.at[dc, rows], ib.at[2], in_s.at[3])),
                (from_over, pltpu.make_async_copy(iy.at[dc, rows], ib.at[3], in_s.at[4]))]

    def sum_load(other, zd, piece):
        dc, rows, _, from_below, from_above, from_over = target(other, zd, piece)
        for cond, sem, buf in ((from_below, lo_r, lo), (from_above, hi_r, hi), (from_over, iy_r, iy)):
            @pl.when(cond)
            def _():
                arrived(sem.at[dc, piece], buf.at[dc, rows])
        for cond, cp in sum_loads(other, zd, piece):
            @pl.when(cond)
            def _():
                cp.start()

    def out_wait(slot):
        pltpu.make_async_copy(ob.at[slot], ob.at[slot], ob_s.at[slot]).wait()

    def sum_send(other, zd, piece, n):
        dc, rows, along, from_below, from_above, from_over = target(other, zd, piece)
        slot = lax.rem(n, SLOTS)
        for cond, cp in sum_loads(other, zd, piece):
            @pl.when(cond)
            def _():
                cp.wait()

        @pl.when(n >= SLOTS)
        def _():
            out_wait(slot)
        for i, cond in ((1, from_below), (2, from_above), (3, from_over)):
            @pl.when(cond)
            def _():
                pb[...] = pb[...] + ib[i].astype(F32)
        ob[slot] = (pb[...] + ib[0].astype(F32)).astype(BF)
        here = along & (zd == z)
        sem = ob_s.at[slot]

        @pl.when(along & (zd > z))
        def _():
            remote(ob.at[slot], lo.at[dc, rows], sem, lo_r.at[dc, piece], above).start()

        @pl.when(along & (zd < z))
        def _():
            remote(ob.at[slot], hi.at[dc, rows], sem, hi_r.at[dc, piece], below).start()

        @pl.when(jnp.logical_not(along) | (here & (other == 1)))
        def _():
            remote(ob.at[slot], iy.at[dc, rows], sem, iy_r.at[dc, piece], across).start()

        @pl.when(here & (other == 0))
        def _():
            pltpu.make_async_copy(ob.at[slot], dx.at[rows], sem).start()

    for cp in down_loads(0, 0):
        cp.start()
    greet(y, z, c)
    for cond, cp in own_hops:
        @pl.when(cond)
        def _():
            cp.start()
    tables = packed(ENDS), packed(INNER)

    def item(i, carry):
        u, n, held = carry
        word = jnp.where(end, *(chosen(t, i // PER) for t in tables))
        code = lax.rem(word, BASE)
        for j in range(1, PER):
            code = jnp.where(lax.rem(i, PER) == j, lax.rem(word // BASE**j, BASE), code)

        def piece_of(index):
            return index // 16, real(lax.rem(index // 4, 4)), lax.rem(index, 4)

        @pl.when(code == 0)
        def _():
            unit(u)
        for part in PARTS:
            @pl.when((code > 0) & (code < SUMS) & (lax.rem(code + 2, 3) == part))
            def _():
                pass_on((code - 1) // 12, real(lax.rem((code - 1) // 3, 4)), part)

        @pl.when((code >= SUMS) & (code < ADD))
        def _():
            sum_load(*piece_of(code - SUMS))

        @pl.when(code == ADD)
        def _():
            sum_send(*piece_of(held), n)
        loaded = (code >= SUMS) & (code < ADD)
        return u + jnp.where(code == 0, 1, 0), n + jnp.where(code == ADD, 1, 0), jnp.where(loaded, code - SUMS, held)

    lax.fori_loop(0, ITEMS, item, (jnp.int32(0),) * 3)

    for slot in range(SLOTS):
        out_wait(slot)

    def drain(n, carry):
        other, zs = n // 4, lax.rem(n, 4)

        @pl.when((other == 1) | (zs != z))
        def _():
            for part in PARTS:
                for cond, cp in x_sends(other, zs, part):
                    @pl.when(cond)
                    def _():
                        cp.wait_send()
        return carry
    lax.fori_loop(0, RING, drain, 0)
    for cond, cp in own_hops:
        @pl.when(cond)
        def _():
            cp.wait_send()


def reduce_call(xf, h, dyf, dgu, pf, qb):
    sd = jax.ShapeDtypeStruct
    hbm = pl.BlockSpec(memory_space=pl.ANY)
    land = sd((RING, R, D), BF)
    outs = [sd((16 * R, D), BF), land, land, land, sd((R, D), BF), sd((D, F), BF), sd((D, F), BF), sd((F, D), BF)]
    dma = pltpu.SemaphoreType.DMA
    return pl.pallas_call(
        reduce_kernel,
        out_shape=outs,
        in_specs=[hbm] * 6,
        out_specs=[hbm] * len(outs),
        input_output_aliases={0: 0},
        scratch_shapes=[
            pltpu.VMEM((D, 2 * F), F32), pltpu.VMEM((2, BLK, D), BF), pltpu.VMEM((2, BLK, 2 * F), BF),
            pltpu.VMEM((2, CAST, D), BF), pltpu.VMEM((PIECE, D), F32), pltpu.VMEM((4, PIECE, D), BF),
            pltpu.VMEM((SLOTS, PIECE, D), BF),
            dma((RING, 3)), dma((3, RING, 3)), dma((RING, 3)), dma((RING, 3)),
            dma((RING, 4)), dma((RING, 4)), dma((RING, 4)), dma((SLOTS,)), dma((2, 4)), dma((2, 2)), dma((5,)),
        ],
        compiler_params=pltpu.CompilerParams(collective_id=1, has_side_effects=True, vmem_limit_bytes=66_000_000),
        cost_estimate=pl.CostEstimate(flops=3 * 2 * 16 * R * D * F, bytes_accessed=300_000_000, transcendentals=0),
        name="reduce",
    )(xf, h, dyf, dgu, pf, qb)


def copy_kernel(*refs):
    n = len(refs) // 2
    for a, b in zip(refs[:n], refs[n:]):
        b[...] = a[...]


COPIES = 6


def copy_call(dx, og, ou, od):
    n = COPIES
    specs = [pl.BlockSpec((R, D // n), lambda i: (0, i)), pl.BlockSpec((D // n, F), lambda i: (i, 0)),
             pl.BlockSpec((D // n, F), lambda i: (i, 0)), pl.BlockSpec((F // n, D), lambda i: (i, 0))]
    return pl.pallas_call(
        copy_kernel,
        grid=(n,),
        out_shape=[jax.ShapeDtypeStruct(a.shape, a.dtype) for a in (dx, og, ou, od)],
        in_specs=specs,
        out_specs=specs,
        compiler_params=pltpu.CompilerParams(dimension_semantics=("arbitrary",), vmem_limit_bytes=66_000_000),
        cost_estimate=pl.CostEstimate(flops=1_000_000, bytes_accessed=61_000_000, transcendentals=0),
        name="copy",
    )(dx, og, ou, od)


def solution(mesh):
    def body(x, dy, gate, up, w_gate, w_up, w_down):
        h, dyf, dgu, pf, qb, xf = back_call(x, dy, gate, up, w_down, w_gate, w_up)
        outs = reduce_call(xf, h, dyf, dgu, pf, qb)
        return tuple(copy_call(*outs[4:]))

    rows, cols = P(("dp", "tp")), P("dp", "tp")
    return jax.shard_map(
        body, mesh=mesh,
        in_specs=(rows, rows, cols, cols, P(None, "tp"), P(None, "tp"), P("tp")),
        out_specs=(rows, cols, cols, P(("dp", "tp"))),
        check_vma=False,
    )
```

```python
import jax
import jax.numpy as jnp
from jax import lax
from jax.experimental import pallas as pl
from jax.experimental.pallas import tpu as pltpu
from jax.sharding import PartitionSpec as P

R, D, F = 352, 3072, 1536
H = R // 2
RING = 8
NC = 2
CH = F
BF, F32 = jnp.bfloat16, jnp.float32
NT = (((1,), (1,)), ((), ()))
C0, C1 = 0.7978845608028654, 0.044715
TILE = 512
KB = 4 * H


def grads(g, u, dh):
    g, u = g.astype(F32), u.astype(F32)
    g2 = g * g
    t = jnp.tanh(g * (C0 + (C0 * C1) * g2))
    q = 0.5 + 0.5 * t
    gelu = g * q
    slope = q + gelu * ((1.0 - q) * (2.0 * C0 + (6.0 * C0 * C1) * g2))
    return (dh * (u * slope)).astype(BF), (dh * gelu).astype(BF), (gelu * u).astype(BF)


MESH = pl.DeviceIdType.MESH
FLOPS, BYTES = 6 * 16 * R * D * F, 300_000_000
TOKENS = 16 * R
VMEM = 66_000_000


def place():
    tp = lax.axis_index("tp")
    y, z, c = tp // 8, lax.rem(tp // 2, 4), lax.rem(tp, 2)
    return y, z, c, jnp.where(y == 0, z, 7 - z)


def chip(y, z, core):
    return (y * 4 + z) * 2 + core


def dev(p, core):
    return chip(p // 4, jnp.where(p < 4, p, 7 - p), core)


def start(pos, s, side, core):
    p = lax.rem(pos + RING - s, RING) if side == 0 else lax.rem(pos + s, RING)
    return pl.multiple_of(dev(p, core) * R + side * H, 16)


def mirrored(z):
    return jnp.where(z < 2, z, 3 - z)


def order(zt, other, zs):
    k = jnp.where(zt < 2, zs, 3 - zs)
    o = jnp.where((mirrored(zt) == 1) & (k < 2), 1 - k, k)
    return 2 * o + other


def home(zs):
    return jnp.where(zs == 0, 1, jnp.where(zs == 3, 2, zs))


def greet(y, z, c):
    bar = pltpu.get_barrier_semaphore()

    def hello(d):
        pl.semaphore_signal(bar, inc=1, device_id={"tp": d}, device_id_type=MESH)
    hello(chip(y, z, 1 - c))
    hello(chip(1 - y, z, c))

    @pl.when(z < 3)
    def _():
        hello(chip(y, z + 1, c))

    @pl.when(z > 0)
    def _():
        hello(chip(y, z - 1, c))
    pl.semaphore_wait(bar, 2 + jnp.where(z < 3, 1, 0) + jnp.where(z > 0, 1, 0))


def remote(src, dst, ss, rs, d):
    return pltpu.make_async_remote_copy(src, dst, ss, rs, device_id={"tp": d}, device_id_type=MESH)


def arrived(sem, dst):
    pltpu.make_async_copy(dst, dst, sem).wait()


XPARTS = ((0, 176), (176, 88), (264, 88))
PARTS = (0, 1, 2)
CROSS = 2
PIECE = 88
BOTH = (0, 1)


def xplace(zt, other, zs, part, mine):
    r0, n = XPARTS[part]
    return pl.ds(pl.multiple_of(order(zt, other, zs) * KB + (0 if mine else R) + r0, 8), n)


def back_kernel(x, dy, gate, up, wd, wg, wu,
                h, dyf, dgo, pf, qb, xf,
                wdv, wgu, dyb, gb, ub, dgu, hb, pv, qs,
                w_s, ld_s, own_s, o_s, p_s, ag_r, ag_t, dd_r, dd_t, q_r, q_t, x_r, x_t):
    y, z, c, pos = place()
    right, left, mate = dev(lax.rem(pos + 1, RING), c), dev(lax.rem(pos + RING - 1, RING), c), dev(pos, 1 - c)
    dirs = (right, left)

    def rows(s, side, core):
        return pl.ds(start(pos, s, side, core), H)

    def slab(s, side, part, mine):
        return dyf.at[pl.ds(pl.multiple_of(s * KB + (0 if mine else R) + side * H + part * PIECE, 8), PIECE)]

    def block(s, mine):
        return pl.ds(pl.multiple_of(s * KB + (0 if mine else R), 16), R)

    def ring_copy(src, s, side, part):
        return remote(src, slab(s, side, part, True), ag_t.at[s, side, part], ag_r.at[s, side, part], dirs[side])

    def mate_copy(src, s, side, part):
        return remote(src, slab(s, side, part, False), dd_t.at[s, side, part], dd_r.at[s, side, part], mate)

    weights = [pltpu.make_async_copy(wd, wdv, w_s.at[0]),
               pltpu.make_async_copy(wg, wgu.at[:, pl.ds(0, F)], w_s.at[1]),
               pltpu.make_async_copy(wu, wgu.at[:, pl.ds(F, F)], w_s.at[2])]

    def loads(s, slot, first=False):
        core = c if slot == 1 else 1 - c
        out = [pltpu.make_async_copy(dy if first else dyf.at[block(s, slot == 1)], dyb.at[slot], ld_s.at[slot, 4])]
        for side in BOTH:
            half, r = pl.ds(side * H, H), rows(s, side, core)
            out += [pltpu.make_async_copy(gate.at[r], gb.at[slot, half], ld_s.at[slot, 2 * side]),
                    pltpu.make_async_copy(up.at[r], ub.at[slot, half], ld_s.at[slot, 2 * side + 1])]
        return out

    def stores(s, slot):
        out = [pltpu.make_async_copy(hb, h.at[block(s, slot == 1)], o_s.at[2])]
        for side in BOTH:
            p = lax.rem(pos + RING - s, RING) if side == 0 else lax.rem(pos + s, RING)
            zs = jnp.where(p < 4, p, 7 - p)
            other = jnp.where(p // 4 == y, 0, 1)
            to = order(z, other, zs) * KB + (0 if slot == 1 else R) + side * H
            out.append(pltpu.make_async_copy(dgu.at[pl.ds(side * H, H)], dgo.at[pl.ds(pl.multiple_of(to, 16), H)],
                                             o_s.at[side]))
        return out

    def dhidden(slot):
        a = dyb[slot]
        for n in range(F // TILE):
            cs = pl.ds(n * TILE, TILE)
            dh = lax.dot_general(a, wdv[n * TILE:(n + 1) * TILE, :], NT, preferred_element_type=F32)
            dg, du, hid = grads(gb[slot, :, cs], ub[slot, :, cs], dh)
            dgu[:, cs] = dg
            dgu[:, pl.ds(F + n * TILE, TILE)] = du
            hb[:, cs] = hid

    def partial_dx(j, store):
        a = dgu[...]
        for n in range(CH // TILE):
            r0 = j * CH + n * TILE
            store(r0, lax.dot_general(a, wgu[r0:r0 + TILE, :], NT, preferred_element_type=F32))

    def q_send(s, j):
        return remote(qs.at[j], qb.at[s, :, pl.ds(j * CH, CH)], q_t.at[j], q_r.at[s, j], mate)

    def p_store(s, j):
        cols = pl.ds(j * CH, CH)
        return pltpu.make_async_copy(pv.at[:, cols], pf.at[s, :, cols], p_s.at[j])

    inner = home(z) == z
    over = chip(1 - y, z, c)
    ways = ((z < 3, chip(y, z + 1, c), 0, z + 1), (z > 0, chip(y, z - 1, c), 0, z - 1), (z >= 0, over, 1, z))
    comes = (z > 0, z < 3, z >= 0)

    def first_hop(w, part, there):
        if w == 3:
            return z >= 0
        if w == 2:
            return inner if part == CROSS else there[w]
        return there[w] if part != 1 else z < 0

    def x_send(w, part):
        r0, n = XPARTS[part]
        src = x.at[pl.ds(r0, n)]
        if w == 3:
            return remote(src, xf.at[xplace(z, 0, z, part, False)], x_t.at[w, part], x_r.at[w, part], mate)
        _, target, other, zt = ways[w]
        return remote(src, xf.at[xplace(zt, other, z, part, True)], x_t.at[w, part], x_r.at[w, part], target)

    zc = jnp.where(z == 1, 0, 3)
    crossing = remote(xf.at[xplace(z, 0, zc, CROSS, True)], xf.at[xplace(z, 1, zc, CROSS, True)],
                      x_t.at[4, CROSS], x_r.at[4, CROSS], over)

    def x_here(w, part):
        arrived(x_r.at[w, part], xf.at[pl.ds(0, XPARTS[part][1])])

    def cross():
        for w, zi in ((0, 1), (1, 2)):
            @pl.when(z == zi)
            def _():
                x_here(w, CROSS)
                crossing.start()

    weights[0].start()
    for cp in loads(0, 1, True):
        cp.start()
    own_x = [pltpu.make_async_copy(x, dyb.at[0], own_s.at[0]),
             pltpu.make_async_copy(dyb.at[0], xf.at[pl.ds(pl.multiple_of(order(z, 0, z) * KB, 16), R)], own_s.at[0])]
    own_x[0].start()
    own_dy = pltpu.make_async_copy(dyb.at[1], dyf.at[pl.ds(0, R)], own_s.at[1])
    greet(y, z, c)

    for part in BOTH:
        for side in BOTH:
            src = dy.at[pl.ds(side * H + part * PIECE, PIECE)]
            ring_copy(src, 1, side, part).start()
            mate_copy(src, 0, side, part).start()

    weights[0].wait()
    weights[1].start()
    weights[2].start()
    own_x[0].wait()
    own_x[1].start()

    def advance(s, part):
        @pl.when(s < RING - 1)
        def _():
            for side in BOTH:
                p = slab(s + 1, side, part, True)
                arrived(ag_r.at[s + 1, side, part], p)

                @pl.when(s < RING - 2)
                def _():
                    ring_copy(p, s + 2, side, part).start()
                mate_copy(p, s + 1, side, part).start()

    def x_leaves():
        for part in reversed(PARTS):
            for w in range(4):
                @pl.when(first_hop(w, part, [way[0] for way in ways]))
                def _():
                    x_send(w, part).start()

    def step(s, carry):
        for cp in loads(s, 1):
            cp.wait()

        @pl.when(s == 0)
        def _():
            own_dy.start()

        @pl.when(s > 0)
        def _():
            for cp in stores(s, 0):
                cp.wait()
            for j in range(NC):
                p_store(s, j).wait()
        dhidden(1)
        for cp in stores(s, 1):
            cp.start()

        @pl.when(s == 0)
        def _():
            own_dy.wait()
            own_x[1].wait()
            weights[1].wait()
            weights[2].wait()

        @pl.when(s < RING - 1)
        def _():
            for cp in loads(s + 1, 1)[1:]:
                cp.start()
        for part in BOTH:
            for side in BOTH:
                arrived(dd_r.at[s, side, part], slab(s, side, part, False))
        for cp in loads(s, 0):
            cp.start()

        def put_p(c0, v):
            pv[:, pl.ds(c0, TILE)] = v
        for j in range(NC):
            partial_dx(j, put_p)
            p_store(s, j).start()
        advance(s, 0)

        @pl.when(s == RING - 1)
        def _():
            cross()

        for cp in loads(s, 0):
            cp.wait()
        for cp in stores(s, 1):
            cp.wait()

        @pl.when(s > 0)
        def _():
            for j in range(NC):
                q_send(s, j).wait_send()

        def put_q(c0, v):
            qs[c0 // CH, :, pl.ds(c0 % CH, TILE)] = v.astype(BF)
        dhidden(0)
        partial_dx(0, put_q)
        for cp in stores(s, 0):
            cp.start()
        q_send(s, 0).start()
        advance(s, 1)

        @pl.when(s < RING - 1)
        def _():
            loads(s + 1, 1)[0].start()

        @pl.when(s == XSTEP)
        def _():
            x_leaves()
        partial_dx(1, put_q)
        q_send(s, 1).start()
        return carry

    lax.fori_loop(0, RING, step, 0)

    for cp in stores(RING - 1, 0):
        cp.wait()
    for j in range(NC):
        p_store(0, j).wait()
        q_send(0, j).wait_send()
    for part in PARTS:
        for w in range(4):
            took = first_hop(w, part, comes)
            if part == CROSS and w < 2:
                took = took & (z != w + 1)

            @pl.when(took)
            def _():
                x_here(w, part)

            @pl.when(first_hop(w, part, [way[0] for way in ways]))
            def _():
                x_send(w, part).wait_send()

    @pl.when(inner)
    def _():
        x_here(4, CROSS)
        crossing.wait_send()

    def drain(s, carry):
        for part in BOTH:
            for side in BOTH:
                p = slab(0, side, part, True)

                @pl.when(s > 0)
                def _():
                    ring_copy(p, s, side, part).wait_send()
                mate_copy(p, s, side, part).wait_send()
        for j in range(NC):
            arrived(q_r.at[s, j], qb.at[0, :, pl.ds(j * CH, CH)])
        return carry
    lax.fori_loop(0, RING, drain, 0)


XSTEP = 5


def back_call(x, dy, gate, up, wd, wg, wu):
    sd = jax.ShapeDtypeStruct
    hbm = pl.BlockSpec(memory_space=pl.ANY)
    outs = [sd((TOKENS, F), BF), sd((TOKENS, D), BF), sd((TOKENS, 2 * F), BF), sd((RING, R, D), F32),
            sd((RING, R, D), BF), sd((TOKENS, D), BF)]
    dma = pltpu.SemaphoreType.DMA
    return pl.pallas_call(
        back_kernel,
        out_shape=outs,
        in_specs=[hbm] * 7,
        out_specs=[hbm] * len(outs),
        scratch_shapes=[
            pltpu.VMEM((F, D), BF), pltpu.VMEM((D, 2 * F), BF),
            pltpu.VMEM((2, R, D), BF), pltpu.VMEM((2, R, F), BF), pltpu.VMEM((2, R, F), BF),
            pltpu.VMEM((R, 2 * F), BF), pltpu.VMEM((R, F), BF),
            pltpu.VMEM((R, D), F32), pltpu.VMEM((NC, R, CH), BF),
            dma((3,)), dma((2, 5)), dma((2,)), dma((3,)), dma((NC,)),
            *[dma((RING, 2, 2))] * 4,
            dma((RING, NC)), dma((NC,)), dma((5, 3)), dma((5, 3)),
        ],
        compiler_params=pltpu.CompilerParams(collective_id=0, has_side_effects=True, vmem_limit_bytes=VMEM),
        cost_estimate=pl.CostEstimate(flops=FLOPS, bytes_accessed=BYTES, transcendentals=TOKENS * F),
        name="back",
    )(x, dy, gate, up, wd, wg, wu)


TN = (((0,), (0,)), ((), ()))
BLK = 512
NB = 16 * R // BLK
WIDE = 256
CAST = 128
SLOTS = 6
TALL = 768
TALLS = F // TALL
DOWN = NB * TALLS
DOWN_OUT = DOWN + 2
GU = 2 * DOWN
GU_OUT = 4
ENDS = "".join((
    "DMFN2ZYyZYZZ4ZEYuZYZZZPmZYZZ0GQZYiZYZZRoZYZZZOeZYZ",
    "ZwZSIY3ZYZ5ZHYkZYZZZgZYZZsZJTYzZYZZZUpZYZZZXvZYZZ1",
    "ZVLYnZYZxZKYjZYZZZlZYZZqZWYcYfYZZtZYhZYZZaZYrZYZZd",
    "ZYZZZbY",
))
INNER = "".join((
    "AGROCIPQZZZZZBHZZZZMZZZZJZZZZUSZZZZXNZZZ2ZLTYZZyZY",
    "4ZKYZZmZYZVZZiZY0ZWYZZ3ZYuZYZZoZYsZYZkZYqZY5ZYeZYz",
    "ZYcZY1ZZYaZYpZYtZYwZYrZYnZYZvZYjZYdZYxZYZlZYbZYgZY",
    "fZYZZhY",
))
LETTERS = "ZABCDEFGHIJKLMNOPQRSTUVWXabcdefghijklmnopqrstuvwxyz012345Y"
SUMS = LETTERS.index("a")
ADD = LETTERS.index("Y")
BASE = 64
PER = 5
ITEMS = len(ENDS)


def packed(work):
    codes = [LETTERS.index(w) for w in work] + [0] * (-len(work) % PER)
    return [sum(code * BASE**j for j, code in enumerate(codes[i:i + PER])) for i in range(0, len(codes), PER)]


def chosen(table, i):
    v = table[0]
    for n, entry in enumerate(table[1:], 1):
        v = jnp.where(i == n, entry, v)
    return v


def reduce_kernel(xin, h, dyf, dgu, pf, qb,
                  xf, lo, hi, iy, dx, og, ou, od,
                  acc, xs, ds, st, pb, ib, ob,
                  x_r, x_t, xd_r, xd_t, lo_r, hi_r, iy_r, ob_s, ld_s, st_s, in_s):
    y, z, c, pos = place()
    end = mirrored(z) == 0
    above, below, across, mate = chip(y, z + 1, c), chip(y, z - 1, c), chip(1 - y, z, c), chip(y, z, 1 - c)

    def real(k):
        return jnp.where(z < 2, k, 3 - k)

    def hop_up(other, zs, part):
        src = xf.at[xplace(z, other, zs, part, True)]
        return remote(src, xf.at[xplace(z + 1, other, zs, part, True)], x_t.at[0, other * 4 + zs, part],
                      x_r.at[other * 4 + zs, part], above)

    def hop_down(other, zs, part):
        src = xf.at[xplace(z, other, zs, part, True)]
        return remote(src, xf.at[xplace(z - 1, other, zs, part, True)], x_t.at[1, other * 4 + zs, part],
                      x_r.at[other * 4 + zs, part], below)

    def x_sends(other, zs, part):
        src = xf.at[xplace(z, other, zs, part, True)]
        n = other * 4 + zs
        if part == CROSS:
            root = jnp.where(other == 0, zs, home(zs))
            turn = (other == 1) & (root == z)
            go_up, go_down = (root < z) | turn, (root > z) | turn
        else:
            go_up, go_down = (other == 0) & (zs < z), (other == 0) & (zs > z)
        out = [(go_up & (z < 3), hop_up(other, zs, part)), (go_down & (z > 0), hop_down(other, zs, part)),
               (z >= 0, remote(src, xf.at[xplace(z, other, zs, part, False)], xd_t.at[n, part], xd_r.at[n, part], mate))]
        if part != CROSS:
            out.append((other == 0, remote(src, xf.at[xplace(z, 1 - other, zs, part, True)], x_t.at[2, n, part],
                                           x_r.at[(1 - other) * 4 + zs, part], across)))
        return out

    def pass_on(other, zs, part):
        near = (other == 0) & ((zs - z) * (zs - z) == 1)
        if part == 0:
            first = near | ((other == 1) & (zs == z))
        elif part == 1:
            first = (other == 1) & (zs == z)
        else:
            first = near | ((other == 1) & (home(zs) == z))

        @pl.when(jnp.logical_not(first))
        def _():
            arrived(x_r.at[other * 4 + zs, part], xf.at[xplace(z, other, zs, part, True)])
        for cond, cp in x_sends(other, zs, part):
            @pl.when(cond)
            def _():
                cp.start()

    own_hops = ((z < 3, hop_up(0, z, 1)), (z > 0, hop_down(0, z, 1)))

    def slot_from_mate(sl, carry):
        o, other = sl // 2, lax.rem(sl, 2)
        k = jnp.where(end | (o > 1), o, 1 - o)
        for part in PARTS:
            arrived(xd_r.at[other * 4 + real(k), part], xf.at[pl.ds(0, XPARTS[part][1])])
        return carry

    def down_loads(b, slot):
        r = pl.ds(pl.multiple_of(b * BLK, 16), BLK)
        return [pltpu.make_async_copy(h.at[r], xs.at[slot, :, pl.ds(0, F)], ld_s.at[slot, 0]),
                pltpu.make_async_copy(dyf.at[r], ds.at[slot], ld_s.at[slot, 1])]

    def loads(b, slot):
        r = pl.ds(pl.multiple_of(b * BLK, 16), BLK)
        return [pltpu.make_async_copy(xf.at[r], xs.at[slot], ld_s.at[slot, 2]),
                pltpu.make_async_copy(dgu.at[r], ds.at[slot], ld_s.at[slot, 3])]

    def product(slot, m, first):
        rows = pl.ds(pl.multiple_of(m * TALL, TALL), TALL)
        a = xs[slot, :, rows]
        for n in range(2 * F // WIDE):
            cols = pl.ds(n * WIDE, WIDE)
            r = lax.dot_general(a, ds[slot, :, cols], TN, preferred_element_type=F32)
            acc[rows, cols] = jnp.where(first, 0.0, acc[rows, cols]) + r

    def last_slot(b):
        return (BLK * (b + 1) - 1) // KB

    def down_copy(i, slot):
        return [pltpu.make_async_copy(st.at[slot], od.at[pl.ds(pl.multiple_of(i * CAST, 16), CAST)], st_s.at[slot, 0])]

    def weight_copies(i, slot):
        r = pl.ds(pl.multiple_of(i * CAST, 16), CAST)
        return [pltpu.make_async_copy(st.at[slot, :, pl.ds(0, F)], og.at[r], st_s.at[slot, 0]),
                pltpu.make_async_copy(st.at[slot, :, pl.ds(F, F)], ou.at[r], st_s.at[slot, 1])]

    def cast(n, part, parts, copies):
        def one(i, carry):
            slot = lax.rem(i, 2)

            @pl.when(i > 1)
            def _():
                for cp in copies(i, slot):
                    cp.wait()
            st[slot] = acc[pl.ds(pl.multiple_of(i * CAST, 16), CAST), :].astype(BF)
            for cp in copies(i, slot):
                cp.start()
            return carry
        lax.fori_loop(part * (n // parts), (part + 1) * (n // parts), one, 0)

        @pl.when(part == parts - 1)
        def _():
            for i in (n - 2, n - 1):
                for cp in copies(i, i % 2):
                    cp.wait()

    def unit(u):
        v = u - DOWN_OUT
        gu = (v >= 0) & (v < GU)
        b = jnp.where(gu, v // (2 * TALLS), u // TALLS)
        m = jnp.where(gu, lax.rem(v, 2 * TALLS), lax.rem(u, TALLS))
        slot = lax.rem(b + jnp.where(gu, NB, 0), 2)

        @pl.when((u < DOWN) & (m == 0))
        def _():
            for cp in down_loads(b, slot):
                cp.wait()

            @pl.when(b < NB - 1)
            def _():
                for cp in down_loads(b + 1, 1 - slot):
                    cp.start()

            @pl.when(b == NB - 1)
            def _():
                for cp in loads(0, 1 - slot):
                    cp.start()

        @pl.when(gu & (m == 0))
        def _():
            for cp in loads(b, slot):
                cp.wait()

        @pl.when(gu & (m == TALLS) & (b < NB - 1))
        def _():
            lax.fori_loop(last_slot(b) + 1, last_slot(b + 1) + 1, slot_from_mate, 0)
            for cp in loads(b + 1, 1 - slot):
                cp.start()

        @pl.when((u < DOWN) | gu)
        def _():
            product(slot, m, b == 0)

        @pl.when((u >= DOWN) & (v < 0))
        def _():
            cast(F // CAST, u - DOWN, DOWN_OUT - DOWN, down_copy)

        @pl.when(v >= GU)
        def _():
            cast(D // CAST, v - GU, GU_OUT, weight_copies)

    def target(other, zd, piece):
        yd = jnp.where(other == 0, y, 1 - y)
        along = (piece < 2) | (other == 0)
        from_below = along & (z > 0) & (zd >= z)
        from_above = along & (z < 3) & (zd <= z)
        from_over = (other == 0) & ((piece > 1) | (zd == z))
        return yd * 4 + zd, pl.ds(pl.multiple_of(piece * PIECE, 8), PIECE), along, from_below, from_above, from_over

    def sum_loads(other, zd, piece):
        dc, rows, _, from_below, from_above, from_over = target(other, zd, piece)
        pd = jnp.where(dc < 4, zd, 7 - zd)
        s = lax.rem(jnp.where(piece < 2, pos - pd, pd - pos) + RING, RING)
        return [(z >= 0, pltpu.make_async_copy(pf.at[s, rows], pb, in_s.at[0])),
                (z >= 0, pltpu.make_async_copy(qb.at[s, rows], ib.at[0], in_s.at[1])),
                (from_below, pltpu.make_async_copy(lo.at[dc, rows], ib.at[1], in_s.at[2])),
                (from_above, pltpu.make_async_copy(hi.at[dc, rows], ib.at[2], in_s.at[3])),
                (from_over, pltpu.make_async_copy(iy.at[dc, rows], ib.at[3], in_s.at[4]))]

    def sum_load(other, zd, piece):
        dc, rows, _, from_below, from_above, from_over = target(other, zd, piece)
        for cond, sem, buf in ((from_below, lo_r, lo), (from_above, hi_r, hi), (from_over, iy_r, iy)):
            @pl.when(cond)
            def _():
                arrived(sem.at[dc, piece], buf.at[dc, rows])
        for cond, cp in sum_loads(other, zd, piece):
            @pl.when(cond)
            def _():
                cp.start()

    def out_wait(slot):
        pltpu.make_async_copy(ob.at[slot], ob.at[slot], ob_s.at[slot]).wait()

    def sum_send(other, zd, piece, n):
        dc, rows, along, from_below, from_above, from_over = target(other, zd, piece)
        slot = lax.rem(n, SLOTS)
        for cond, cp in sum_loads(other, zd, piece):
            @pl.when(cond)
            def _():
                cp.wait()

        @pl.when(n >= SLOTS)
        def _():
            out_wait(slot)
        for i, cond in ((1, from_below), (2, from_above), (3, from_over)):
            @pl.when(cond)
            def _():
                pb[...] = pb[...] + ib[i].astype(F32)
        ob[slot] = (pb[...] + ib[0].astype(F32)).astype(BF)
        here = along & (zd == z)
        sem = ob_s.at[slot]

        @pl.when(along & (zd > z))
        def _():
            remote(ob.at[slot], lo.at[dc, rows], sem, lo_r.at[dc, piece], above).start()

        @pl.when(along & (zd < z))
        def _():
            remote(ob.at[slot], hi.at[dc, rows], sem, hi_r.at[dc, piece], below).start()

        @pl.when(jnp.logical_not(along) | (here & (other == 1)))
        def _():
            remote(ob.at[slot], iy.at[dc, rows], sem, iy_r.at[dc, piece], across).start()

        @pl.when(here & (other == 0))
        def _():
            pltpu.make_async_copy(ob.at[slot], dx.at[rows], sem).start()

    for cp in down_loads(0, 0):
        cp.start()
    greet(y, z, c)
    for cond, cp in own_hops:
        @pl.when(cond)
        def _():
            cp.start()
    tables = packed(ENDS), packed(INNER)

    def item(i, carry):
        u, n, held = carry
        word = jnp.where(end, *(chosen(t, i // PER) for t in tables))
        code = lax.rem(word, BASE)
        for j in range(1, PER):
            code = jnp.where(lax.rem(i, PER) == j, lax.rem(word // BASE**j, BASE), code)

        def piece_of(index):
            return index // 16, real(lax.rem(index // 4, 4)), lax.rem(index, 4)

        @pl.when(code == 0)
        def _():
            unit(u)
        for part in PARTS:
            @pl.when((code > 0) & (code < SUMS) & (lax.rem(code + 2, 3) == part))
            def _():
                pass_on((code - 1) // 12, real(lax.rem((code - 1) // 3, 4)), part)

        @pl.when((code >= SUMS) & (code < ADD))
        def _():
            sum_load(*piece_of(code - SUMS))

        @pl.when(code == ADD)
        def _():
            sum_send(*piece_of(held), n)
        loaded = (code >= SUMS) & (code < ADD)
        return u + jnp.where(code == 0, 1, 0), n + jnp.where(code == ADD, 1, 0), jnp.where(loaded, code - SUMS, held)

    lax.fori_loop(0, ITEMS, item, (jnp.int32(0),) * 3)

    for slot in range(SLOTS):
        out_wait(slot)

    def drain(n, carry):
        other, zs = n // 4, lax.rem(n, 4)

        @pl.when((other == 1) | (zs != z))
        def _():
            for part in PARTS:
                for cond, cp in x_sends(other, zs, part):
                    @pl.when(cond)
                    def _():
                        cp.wait_send()
        return carry
    lax.fori_loop(0, RING, drain, 0)
    for cond, cp in own_hops:
        @pl.when(cond)
        def _():
            cp.wait_send()


def reduce_call(xf, h, dyf, dgu, pf, qb):
    sd = jax.ShapeDtypeStruct
    hbm = pl.BlockSpec(memory_space=pl.ANY)
    land = sd((RING, R, D), BF)
    outs = [sd((TOKENS, D), BF), land, land, land, sd((R, D), BF), sd((D, F), BF), sd((D, F), BF), sd((F, D), BF)]
    dma = pltpu.SemaphoreType.DMA
    return pl.pallas_call(
        reduce_kernel,
        out_shape=outs,
        in_specs=[hbm] * 6,
        out_specs=[hbm] * len(outs),
        input_output_aliases={0: 0},
        scratch_shapes=[
            pltpu.VMEM((D, 2 * F), F32), pltpu.VMEM((2, BLK, D), BF), pltpu.VMEM((2, BLK, 2 * F), BF),
            pltpu.VMEM((2, CAST, D), BF), pltpu.VMEM((PIECE, D), F32), pltpu.VMEM((4, PIECE, D), BF),
            pltpu.VMEM((SLOTS, PIECE, D), BF),
            dma((RING, 3)), dma((3, RING, 3)), dma((RING, 3)), dma((RING, 3)),
            *[dma((RING, 4))] * 3, dma((SLOTS,)), dma((2, 4)), dma((2, 2)), dma((5,)),
        ],
        compiler_params=pltpu.CompilerParams(collective_id=1, has_side_effects=True, vmem_limit_bytes=VMEM),
        cost_estimate=pl.CostEstimate(flops=FLOPS, bytes_accessed=BYTES, transcendentals=0),
        name="reduce",
    )(xf, h, dyf, dgu, pf, qb)


def copy_kernel(*refs):
    n = len(refs) // 2
    for a, b in zip(refs[:n], refs[n:]):
        b[...] = a[...]


COPIES = 6


def copy_call(dx, og, ou, od):
    n = COPIES
    specs = [pl.BlockSpec((R, D // n), lambda i: (0, i)), pl.BlockSpec((D // n, F), lambda i: (i, 0)),
             pl.BlockSpec((D // n, F), lambda i: (i, 0)), pl.BlockSpec((F // n, D), lambda i: (i, 0))]
    return pl.pallas_call(
        copy_kernel,
        grid=(n,),
        out_shape=[jax.ShapeDtypeStruct(a.shape, a.dtype) for a in (dx, og, ou, od)],
        in_specs=specs,
        out_specs=specs,
        compiler_params=pltpu.CompilerParams(dimension_semantics=("arbitrary",), vmem_limit_bytes=VMEM),
        cost_estimate=pl.CostEstimate(flops=1_000_000, bytes_accessed=61_000_000, transcendentals=0),
        name="copy",
    )(dx, og, ou, od)


def solution(mesh):
    def body(x, dy, gate, up, w_gate, w_up, w_down):
        h, dyf, dgu, pf, qb, xf = back_call(x, dy, gate, up, w_down, w_gate, w_up)
        outs = reduce_call(xf, h, dyf, dgu, pf, qb)
        return tuple(copy_call(*outs[4:]))

    rows, cols = P(("dp", "tp")), P("dp", "tp")
    return jax.shard_map(
        body, mesh=mesh,
        in_specs=(rows, rows, cols, cols, P(None, "tp"), P(None, "tp"), P("tp")),
        out_specs=(rows, cols, cols, P(("dp", "tp"))),
        check_vma=False,
    )
```
